128 devices in a mesh: dp: 1, ep: 16 (over z, y), tp: 8 (over x, core).
Axes of the slice: x: 4, y: 4, z: 4, core: 2. Of those that a mesh axis runs over, the one named last changes fastest.
Arguments:
- tokens: bfloat16 [32768, 2048], P(('dp', 'ep', 'tp'))
- expert_ids: int32 [32768, 8], P(('dp', 'ep', 'tp'))
- gate_vals: float32 [32768, 8], P(('dp', 'ep', 'tp'))
- w_gate: bfloat16 [128, 2048, 768], P('ep', None, 'tp')
- w_up: bfloat16 [128, 2048, 768], P('ep', None, 'tp')
- w_down: bfloat16 [128, 768, 2048], P('ep', 'tp')
Outputs:
- output: bfloat16 [32768, 2048], P(('dp', 'ep', 'tp'))
All inputs are finite; a program needn't handle non-finite values.
Results may differ from the reference program's by a relative error of at most 0.010046.
Values are sent between devices in bfloat16 or wider.
A program may use at most 1 GiB of HBM per device.

```python
import jax
import jax.numpy as jnp
from jax import lax

DMODEL = 2048
FFN = 768
EXPERTS = 128
TOP = 8
TOK_LOC = 256
CAP_FACTOR = 2
EXPERT_RANKS = 16
TENSOR_RANKS = 8

NUM_DEV = EXPERT_RANKS * TENSOR_RANKS
CAPACITY = CAP_FACTOR * TOP * TOK_LOC // EXPERTS
HOT_ROWS = CAPACITY + 1


def routing_draw(key_route, key_hot):
    scores = jax.random.randint(key_route, (NUM_DEV, TOK_LOC, EXPERTS), 0, 65536)
    scores = scores * EXPERTS + jnp.arange(EXPERTS, dtype=jnp.int32)
    hot_ids = jax.random.randint(key_hot, (NUM_DEV, 1, 1), 0, EXPERTS)
    forced = (jnp.arange(TOK_LOC)[None, :, None] < HOT_ROWS) & (jnp.arange(EXPERTS)[None, None, :] == hot_ids)
    scores = scores + jnp.where(forced, 16777216, 0)
    chosen = lax.top_k(scores, TOP)[1]
    return chosen.reshape(NUM_DEV * TOK_LOC, TOP).astype(jnp.int32)


def setup_inputs(seed: int = 0, part: int = 0) -> dict:
    subkeys = jax.random.split(jax.random.key(seed), 8)
    key_tok = jax.random.fold_in(subkeys[0], part)
    key_route = jax.random.fold_in(subkeys[1], part)
    key_hot = jax.random.fold_in(subkeys[2], part)
    key_gate = jax.random.fold_in(subkeys[3], part)
    row_count = NUM_DEV * TOK_LOC
    tokens = jax.random.normal(key_tok, (row_count, DMODEL), jnp.float32).astype(jnp.bfloat16)
    expert_ids = routing_draw(key_route, key_hot)
    gate_vals = (0.5 + jax.random.uniform(key_gate, (row_count, TOP), jnp.float32)) * TOP ** -0.5
    w_gate = (jax.random.normal(subkeys[4], (EXPERTS, DMODEL, FFN), jnp.float32) * DMODEL ** -0.5).astype(jnp.bfloat16)
    w_up = (jax.random.normal(subkeys[5], (EXPERTS, DMODEL, FFN), jnp.float32) * DMODEL ** -0.5).astype(jnp.bfloat16)
    w_down = (jax.random.normal(subkeys[6], (EXPERTS, FFN, DMODEL), jnp.float32) * FFN ** -0.5).astype(jnp.bfloat16)
    return {"tokens": tokens, "expert_ids": expert_ids, "gate_vals": gate_vals, "w_gate": w_gate, "w_up": w_up, "w_down": w_down}


def slot_table(ids_one):
    flat_ids = ids_one.reshape(TOK_LOC * TOP)
    one_hot = (flat_ids[:, None] == jnp.arange(EXPERTS, dtype=jnp.int32)[None, :]).astype(jnp.int32)
    preceding = jnp.cumsum(one_hot, axis=0) - one_hot
    return jnp.sum(preceding * one_hot, axis=1).reshape(TOK_LOC, TOP)


def reference(tokens, expert_ids, gate_vals, w_gate, w_up, w_down):
    ids_dev = expert_ids.reshape(NUM_DEV, TOK_LOC, TOP)
    slot_ids = jax.vmap(slot_table)(ids_dev)
    kept_mask = slot_ids < CAPACITY
    dev_index = jnp.arange(NUM_DEV, dtype=jnp.int32)[:, None, None]
    tok_index = dev_index * TOK_LOC + jnp.arange(TOK_LOC, dtype=jnp.int32)[None, :, None] + jnp.zeros_like(slot_ids)
    total_slots = EXPERTS * NUM_DEV * CAPACITY
    dest_slot = jnp.where(kept_mask, (ids_dev * NUM_DEV + dev_index) * CAPACITY + slot_ids, total_slots)
    src_rows = jnp.zeros((total_slots,), jnp.int32).at[dest_slot.reshape(-1)].set(tok_index.reshape(-1), mode="drop")
    src_gate = jnp.zeros((total_slots,), jnp.float32).at[dest_slot.reshape(-1)].set(gate_vals.reshape(-1), mode="drop")

    def expert_step(acc_sum, per_expert):
        rows_idx, row_gate, wg_one, wu_one, wd_one = per_expert
        x_rows = jnp.take(tokens, rows_idx, axis=0)
        gate_pre = jnp.dot(x_rows, wg_one, preferred_element_type=jnp.float32)
        up_pre = jnp.dot(x_rows, wu_one, preferred_element_type=jnp.float32)
        hidden = (jax.nn.silu(gate_pre) * up_pre).astype(jnp.bfloat16)
        y_rows = jnp.dot(hidden, wd_one, preferred_element_type=jnp.float32).astype(jnp.bfloat16)
        acc_sum = acc_sum.at[rows_idx].add(y_rows.astype(jnp.float32) * row_gate[:, None])
        return acc_sum, None

    acc_init = jnp.zeros((NUM_DEV * TOK_LOC, DMODEL), jnp.float32)
    per_rows = src_rows.reshape(EXPERTS, NUM_DEV * CAPACITY)
    per_gate = src_gate.reshape(EXPERTS, NUM_DEV * CAPACITY)
    acc_final, _ = lax.scan(expert_step, acc_init, (per_rows, per_gate, w_gate, w_up, w_down))
    return acc_final.astype(jnp.bfloat16)
```

```python
import jax
import jax.numpy as jnp
from jax import lax
from jax.sharding import PartitionSpec as P

CAP_FACTOR = 2


def slot_map(ids_loc, gate_loc, n_exp, capacity):
    tok_loc = ids_loc.shape[0]
    hit = ids_loc[None, :, :] == jnp.arange(n_exp, dtype=jnp.int32)[:, None, None]
    chosen = jnp.any(hit, axis=2)
    gates = jnp.sum(jnp.where(hit, gate_loc[None], 0.0), axis=2)
    before = (jnp.arange(tok_loc)[:, None] < jnp.arange(tok_loc)[None, :]).astype(jnp.bfloat16)
    slots = jnp.dot(chosen.astype(jnp.bfloat16), before, preferred_element_type=jnp.float32)
    slots = jnp.where(chosen & (slots < capacity), slots, -1.0)
    return slots, gates


def split3(g):
    hi = lax.reduce_precision(g, 8, 7)
    mid = lax.reduce_precision(g - hi, 8, 7)
    lo = g - hi - mid
    return [v.astype(jnp.bfloat16) for v in (hi, mid, lo)]


def solution(mesh):
    expert_ranks = mesh.shape["ep"]
    row_spec = P(("dp", "ep", "tp"), None)

    def local_layer(x_loc, ids_loc, gate_loc, wg_loc, wu_loc, wd_loc):
        tok_loc, d_model = x_loc.shape
        n_top = ids_loc.shape[1]
        local_exp = wg_loc.shape[0]
        n_exp = local_exp * expert_ranks
        capacity = CAP_FACTOR * n_top * tok_loc // n_exp
        wgt = lax.all_gather(jnp.swapaxes(wg_loc, 1, 2), "tp")
        wut = lax.all_gather(jnp.swapaxes(wu_loc, 1, 2), "tp")
        wdt = lax.all_gather(wd_loc, "tp")
        slots, gates = slot_map(ids_loc, gate_loc, n_exp, capacity)
        tok_all = lax.all_gather(x_loc, "ep")
        meta = lax.all_to_all(slots.reshape(expert_ranks, local_exp, tok_loc), "ep", 0, 0, tiled=True)
        cap_iota = jnp.arange(capacity, dtype=jnp.float32)
        pick = (meta[:, :, None, :] == cap_iota[None, None, :, None]).astype(jnp.bfloat16)
        rows = jnp.einsum("sect,std->escd", pick, tok_all, preferred_element_type=jnp.float32).astype(jnp.bfloat16)
        rows = rows.reshape(local_exp, expert_ranks * capacity, d_model)
        gate_pre = jnp.einsum("erd,tefd->ertf", rows, wgt, preferred_element_type=jnp.float32)
        up_pre = jnp.einsum("erd,tefd->ertf", rows, wut, preferred_element_type=jnp.float32)
        hidden = (jax.nn.silu(gate_pre) * up_pre).astype(jnp.bfloat16)
        y_rows = jnp.einsum("ertf,tefd->erd", hidden, wdt, preferred_element_type=jnp.float32).astype(jnp.bfloat16)
        y_rows = y_rows.reshape(local_exp, expert_ranks, capacity, d_model)
        returned = lax.all_to_all(y_rows, "ep", 1, 1, tiled=True)
        mine = slots.reshape(expert_ranks, local_exp, tok_loc)
        place = mine[:, :, None, :] == cap_iota[None, None, :, None]
        acc = 0.0
        for part in split3(gates.reshape(expert_ranks, local_exp, tok_loc)):
            wts = jnp.where(place, part[:, :, None, :], jnp.bfloat16(0))
            acc = acc + jnp.einsum("rect,ercd->td", wts, returned, preferred_element_type=jnp.float32)
        return acc.astype(jnp.bfloat16)

    return jax.shard_map(local_layer, mesh=mesh, in_specs=(row_spec, row_spec, row_spec, P("ep", None, "tp"), P("ep", None, "tp"), P("ep", "tp", None)), out_specs=row_spec, check_vma=False)
```

```python
import functools

import jax
import jax.numpy as jnp
from jax import lax
from jax.experimental import pallas as pl
from jax.experimental.pallas import tpu as pltpu
from jax.sharding import PartitionSpec as P

CAP_FACTOR = 2
RING = 4
CORES = 2
MESH = pl.DeviceIdType.MESH
F32 = jnp.float32
BF16 = jnp.bfloat16


def slot_map(ids_loc, gate_loc, n_exp, capacity):
    tok_loc = ids_loc.shape[0]
    hit = ids_loc[None, :, :] == jnp.arange(n_exp, dtype=jnp.int32)[:, None, None]
    chosen = jnp.any(hit, axis=2)
    gates = jnp.sum(jnp.where(hit, gate_loc[None], 0.0), axis=2)
    before = (jnp.arange(tok_loc)[:, None] < jnp.arange(tok_loc)[None, :]).astype(BF16)
    slots = jnp.dot(chosen.astype(BF16), before, preferred_element_type=F32)
    slots = jnp.where(chosen & (slots < capacity), slots, -1.0)
    return slots, gates


def remote(src, dst, send, recv, **device):
    return pltpu.make_async_remote_copy(src_ref=src, dst_ref=dst, send_sem=send, recv_sem=recv, device_id=device, device_id_type=MESH)


def moe_kernel(n_rank, n_loc, capacity, x_hbm, wg, wu, wd, slots_send, slots_own, gates_own, out, wfull, yret, tok, meta, rows_in, wbuf, ybuf, retbuf, acc, ring_s, ring_r, part_s, part_r, line_s, line_r, plane_s, plane_r, meta_s, meta_r, y_s, y_r, load_sem, own_sem, ret_sem, tok_sem):
    ep = lax.axis_index("ep")
    tp = lax.axis_index("tp")
    z, y = ep // RING, lax.rem(ep, RING)
    x, core = tp // CORES, lax.rem(tp, CORES)
    weights = (wg, wu, wd)
    cols = wg.shape[1]
    half = cols // 2
    tok_loc = x_hbm.shape[0]
    quart = tok_loc // 4
    n_rows = n_rank * capacity

    def step(pos, amount):
        return lax.rem(pos + amount + 2 * RING, RING)

    ring_to = (step(x, 1) * CORES + core, step(x, -1) * CORES + core)
    partner = x * CORES + 1 - core

    def chunk_rows(t, d):
        return pl.ds(pl.multiple_of(t * cols + d * half, 16), half)

    def ring_in_x(d, s):
        return step(x, -1 - s) if d == 0 else step(x, 1 + s)

    def ring_start(d, s, e):
        if s == 0:
            rows = chunk_rows(tp, d)
            for i, w in enumerate(weights):
                remote(w.at[e, pl.ds(d * half, half), :], wfull.at[e, i, rows, :], ring_s.at[d, s, e], ring_r.at[d, s, e], tp=ring_to[d]).start()
        else:
            piece = wfull.at[e, :, chunk_rows(ring_in_x(d, s - 1) * CORES + core, d), :]
            remote(piece, piece, ring_s.at[d, s, e], ring_r.at[d, s, e], tp=ring_to[d]).start()

    def ring_desc(d, s, e):
        piece = wfull.at[e, :, chunk_rows(ring_in_x(d, s) * CORES + core, d), :]
        return remote(piece, piece, ring_s.at[d, s, e], ring_r.at[d, s, e], tp=ring_to[d])

    def own_rows(t):
        return pl.ds(pl.multiple_of(t * cols, 16), cols)

    def share_own(e):
        for i, w in enumerate(weights):
            remote(w.at[e], wfull.at[e, i, own_rows(tp), :], part_s.at[6, e], part_r.at[6, e], tp=partner).start()

    def share_own_desc(e):
        piece = wfull.at[e, :, own_rows(partner), :]
        return remote(piece, piece, part_s.at[6, e], part_r.at[6, e], tp=partner)

    def share(d, s, e):
        piece = wfull.at[e, :, chunk_rows(ring_in_x(d, s) * CORES + core, d), :]
        remote(piece, piece, part_s.at[d * 3 + s, e], part_r.at[d * 3 + s, e], tp=partner).start()

    def share_desc(d, s, e):
        piece = wfull.at[e, :, chunk_rows(ring_in_x(d, s) * CORES + 1 - core, d), :]
        return remote(piece, piece, part_s.at[d * 3 + s, e], part_r.at[d * 3 + s, e], tp=partner)

    routes = (("y", 1), ("y", -1), ("z", 1), ("z", -1))

    def plane_peer(axis, amount):
        return z * RING + step(y, amount) if axis == "y" else step(z, amount) * RING + y

    def quarter(q):
        return pl.ds(q * quart, quart)

    def line_piece(q, back):
        axis, sign = routes[q]
        if axis == "y":
            return tok.at[z, step(y, -sign * back), quarter(q), :]
        return tok.at[step(z, -sign * back), y, quarter(q), :]

    def line_start(q, s):
        axis, sign = routes[q]
        src = x_hbm.at[quarter(q), :] if s == 0 else line_piece(q, s)
        remote(src, line_piece(q, s), line_s.at[q, s], line_r.at[q, s], ep=plane_peer(axis, sign)).start()

    def line_desc(q, s):
        axis, sign = routes[q]
        piece = line_piece(q, s + 1)
        return remote(piece, piece, line_s.at[q, s], line_r.at[q, s], ep=plane_peer(axis, sign))

    def plane_piece(q, back):
        axis, sign = routes[q]
        if axis == "y":
            return tok.at[step(z, -sign * back), :, quarter(q), :]
        return tok.at[:, step(y, -sign * back), quarter(q), :]

    def plane_start(q, s):
        axis, sign = routes[q]
        piece = plane_piece(q, s)
        remote(piece, piece, plane_s.at[q, s], plane_r.at[q, s], ep=plane_peer("z" if axis == "y" else "y", sign)).start()

    def plane_desc(q, s):
        axis, sign = routes[q]
        piece = plane_piece(q, s + 1)
        return remote(piece, piece, plane_s.at[q, s], plane_r.at[q, s], ep=plane_peer("z" if axis == "y" else "y", sign))

    def peer(j):
        return lax.rem(ep + j, n_rank)

    def back_peer(j):
        return lax.rem(ep + n_rank - j, n_rank)

    def src_rows(r):
        return pl.ds(pl.multiple_of(r * capacity, capacity), capacity)

    def y_send(e, k, j):
        r = peer(j)
        return remote(ybuf.at[k, src_rows(r), :], yret.at[e, ep], y_s.at[k, j], y_r.at[e, j], ep=r)

    def y_recv(e, j):
        r = back_peer(j)
        return remote(yret.at[e, r], yret.at[e, r], y_s.at[0, j], y_r.at[e, j], ep=peer(j))

    def y_own(e, k):
        return pltpu.make_async_copy(ybuf.at[k, src_rows(ep), :], yret.at[e, ep], own_sem.at[k])

    barrier = pltpu.get_barrier_semaphore()
    for j in range(1, n_rank):
        pl.semaphore_signal(barrier, inc=1, device_id={"ep": peer(j)}, device_id_type=MESH)
    for t in (*ring_to, partner):
        pl.semaphore_signal(barrier, inc=1, device_id={"tp": t}, device_id_type=MESH)
    pl.semaphore_wait(barrier, n_rank - 1 + 3)

    def ring_issue(b, static):
        def when(cond, fn):
            if static:
                if cond:
                    fn()
            else:
                pl.when(cond)(fn)

        def first():
            for d in range(2):
                ring_desc(d, 0, b).wait_recv()
                ring_start(d, 1, b)
            for d in range(2):
                share(d, 0, b)

        def second():
            for d in range(2):
                ring_desc(d, 1, b - 1).wait_recv()
                ring_start(d, 2, b - 1)
            for d in range(2):
                share(d, 1, b - 1)

        def ahead():
            for d in range(2):
                ring_start(d, 0, b + 2)
            share_own(b + 2)

        when(b < n_loc, first)
        if static:
            if 1 <= b:
                second()
        else:
            pl.when(b <= n_loc)(second)
        when(b + 2 < n_loc, ahead)

    def combine(e):
        for j in range(1, n_rank):
            y_recv(e, j).wait_recv()
        y_own(e, lax.rem(e, 2)).wait()
        load = pltpu.make_async_copy(yret.at[e], retbuf, ret_sem)
        load.start()
        slot_iota = lax.broadcasted_iota(jnp.int32, (n_rank, capacity, tok_loc), 1).astype(F32)
        place = slots_own[e][:, None, :] == slot_iota
        mix = jnp.where(place, gates_own[e][:, None, :], 0.0).reshape(n_rows, tok_loc).T
        hi = mix.astype(BF16)
        rest = mix - hi.astype(F32)
        mid = rest.astype(BF16)
        low = (rest - mid.astype(F32)).astype(BF16)
        load.wait()
        for n in range(4):
            width = acc.shape[1] // 4
            blk = pl.ds(n * width, width)
            ret = retbuf[:, :, blk].reshape(n_rows, width)
            acc[:, blk] += jnp.dot(hi, ret, preferred_element_type=F32) + jnp.dot(mid, ret, preferred_element_type=F32) + jnp.dot(low, ret, preferred_element_type=F32)

    def expert(e, static_first=False):
        for d in range(2):
            ring_desc(d, 2, e).wait_recv()
            share(d, 2, e)
        share_own_desc(e).wait_recv()
        for d in range(2):
            for s in range(3):
                share_desc(d, s, e).wait_recv()
        copies = []
        for i, w in enumerate(weights):
            copies.append(pltpu.make_async_copy(w.at[e], wbuf.at[i, own_rows(tp), :], load_sem.at[i]))
        for j in range(1, RING * CORES):
            other = own_rows(lax.rem(tp + j, RING * CORES))
            copies.append(pltpu.make_async_copy(wfull.at[e, :, other, :], wbuf.at[:, other, :], load_sem.at[2 + j]))
        for c in copies:
            c.start()
        k = lax.rem(e, 2)

        @pl.when(e >= 2)
        def _():
            for j in range(1, n_rank):
                y_send(e - 2, k, j).wait_send()

        for c in copies:
            c.wait()
        xe = rows_in[e]
        hidden = []
        for f in range(3):
            blk = pl.ds(f * 256, 256)
            dims = (((1,), (1,)), ((), ()))
            a = lax.dot_general(xe, wbuf[0, blk, :], dims, preferred_element_type=F32)
            b = lax.dot_general(xe, wbuf[1, blk, :], dims, preferred_element_type=F32)
            hidden.append((jax.nn.silu(a) * b).astype(BF16))
        h = jnp.concatenate(hidden, axis=1)
        for n in range(4):
            width = ybuf.shape[2] // 4
            blk = pl.ds(n * width, width)
            ybuf[k, :, blk] = jnp.dot(h, wbuf[2, :, blk], preferred_element_type=F32).astype(BF16)
        y_own(e, k).start()
        for j in range(1, n_rank):
            y_send(e, k, j).start()

    for b in range(2):
        for d in range(2):
            ring_start(d, 0, b)
    for q in range(4):
        line_start(q, 0)
    load_own = pltpu.make_async_copy(x_hbm, tok.at[z, y], tok_sem)
    load_own.start()
    for j in range(1, n_rank):
        remote(slots_send.at[peer(j)], meta.at[ep], meta_s.at[j], meta_r.at[j], ep=peer(j)).start()
    for b in range(2):
        share_own(b)
    meta[ep] = slots_send[ep]
    acc[...] = jnp.zeros_like(acc)
    for s in range(2):
        for q in range(4):
            line_desc(q, s).wait_recv()
            line_start(q, s + 1)
    ring_issue(0, True)
    load_own.wait()
    for q in range(4):
        line_desc(q, 2).wait_recv()
    for q in range(4):
        plane_start(q, 0)
    ring_issue(1, True)
    for q in range(4):
        plane_desc(q, 0).wait_recv()
        plane_start(q, 1)
    ring_issue(2, True)
    for q in range(4):
        plane_desc(q, 1).wait_recv()
        plane_start(q, 2)
    for q in range(4):
        plane_desc(q, 2).wait_recv()
    for j in range(1, n_rank):
        remote(slots_send.at[back_peer(j)], meta.at[back_peer(j)], meta_s.at[j], meta_r.at[j], ep=peer(j)).wait_recv()

    @pl.loop(0, n_rank)
    def _(s):
        slot_iota = lax.broadcasted_iota(jnp.int32, (n_loc, capacity, tok_loc), 1).astype(F32)
        pick = jnp.where(meta[s][:, None, :] == slot_iota, 1.0, 0.0).reshape(n_loc * capacity, tok_loc).astype(BF16)
        picked = jnp.dot(pick, tok[s // RING, lax.rem(s, RING)], preferred_element_type=F32).astype(BF16)
        for e in range(n_loc):
            rows_in[e, src_rows(s), :] = picked[e * capacity:(e + 1) * capacity]

    @pl.loop(2, n_loc + 2)
    def _(b):
        @pl.when(b > 2)
        def _():
            ring_issue(b, False)

        expert(b - 2)

        @pl.when(b > 2)
        def _():
            combine(b - 3)

    combine(n_loc - 1)
    out[...] = acc[...].astype(out.dtype)

    for e in (n_loc - 2, n_loc - 1):
        k = e % 2
        for j in range(1, n_rank):
            y_send(e, k, j).wait_send()
    for q in range(4):
        for s in range(3):
            line_desc(q, s).wait_send()
            plane_desc(q, s).wait_send()
    for j in range(1, n_rank):
        remote(slots_send.at[peer(j)], meta.at[ep], meta_s.at[j], meta_r.at[j], ep=peer(j)).wait_send()

    @pl.loop(0, n_loc)
    def _(e):
        share_own_desc(e).wait_send()
        for d in range(2):
            for s in range(3):
                ring_desc(d, s, e).wait_send()
                share_desc(d, s, e).wait_send()


def solution(mesh):
    expert_ranks = mesh.shape["ep"]
    row_spec = P(("dp", "ep", "tp"), None)

    def local_layer(x_loc, ids_loc, gate_loc, wg_loc, wu_loc, wd_loc):
        tok_loc, d_model = x_loc.shape
        n_top = ids_loc.shape[1]
        local_exp, _, cols = wg_loc.shape
        ffn = cols * mesh.shape["tp"]
        n_exp = local_exp * expert_ranks
        capacity = CAP_FACTOR * n_top * tok_loc // n_exp
        n_rows = expert_ranks * capacity
        slots, gates = slot_map(ids_loc, gate_loc, n_exp, capacity)
        slots = slots.reshape(expert_ranks, local_exp, tok_loc)
        gates = gates.reshape(expert_ranks, local_exp, tok_loc)
        any_spec = pl.BlockSpec(memory_space=pl.ANY)
        vmem_spec = pl.BlockSpec(memory_space=pltpu.VMEM)
        dma = pltpu.SemaphoreType.DMA
        out = pl.pallas_call(
            functools.partial(moe_kernel, expert_ranks, local_exp, capacity),
            out_shape=(
                jax.ShapeDtypeStruct((tok_loc, d_model), BF16),
                jax.ShapeDtypeStruct((local_exp, 3, ffn, d_model), BF16),
                jax.ShapeDtypeStruct((local_exp, expert_ranks, capacity, d_model), BF16),
            ),
            in_specs=[any_spec] * 4 + [vmem_spec] * 3,
            out_specs=(vmem_spec, any_spec, any_spec),
            scratch_shapes=[
                pltpu.VMEM((RING, RING, tok_loc, d_model), BF16),
                pltpu.VMEM((expert_ranks, local_exp, tok_loc), F32),
                pltpu.VMEM((local_exp, n_rows, d_model), BF16),
                pltpu.VMEM((3, ffn, d_model), BF16),
                pltpu.VMEM((2, n_rows, d_model), BF16),
                pltpu.VMEM((expert_ranks, capacity, d_model), BF16),
                pltpu.VMEM((tok_loc, d_model), F32),
                dma((2, 3, local_exp)),
                dma((2, 3, local_exp)),
                dma((7, local_exp)),
                dma((7, local_exp)),
                dma((4, 3)),
                dma((4, 3)),
                dma((4, 3)),
                dma((4, 3)),
                dma((expert_ranks,)),
                dma((expert_ranks,)),
                dma((2, expert_ranks)),
                dma((local_exp, expert_ranks)),
                dma((10,)),
                dma((2,)),
                dma,
                dma,
            ],
            compiler_params=pltpu.CompilerParams(collective_id=0, has_side_effects=True, vmem_limit_bytes=67000000),
        )(
            x_loc,
            jnp.swapaxes(wg_loc, 1, 2),
            jnp.swapaxes(wu_loc, 1, 2),
            wd_loc,
            slots,
            jnp.swapaxes(slots, 0, 1),
            jnp.swapaxes(gates, 0, 1),
        )
        return out[0]

    return jax.shard_map(local_layer, mesh=mesh, in_specs=(row_spec, row_spec, row_spec, P("ep", None, "tp"), P("ep", None, "tp"), P("ep", "tp", None)), out_specs=row_spec, check_vma=False)
```

```python
import functools

import jax
import jax.numpy as jnp
from jax import lax
from jax.experimental import pallas as pl
from jax.experimental.pallas import tpu as pltpu
from jax.sharding import PartitionSpec as P

CAP_FACTOR = 2
RING = 4
CORES = 2
MESH = pl.DeviceIdType.MESH
F32 = jnp.float32
BF16 = jnp.bfloat16


ROUND = ((0, 1), (0, -1), (1, 0), (-1, 0), (2, 2), (1, 1), (-1, -1), (1, -1), (-1, 1), (0, 2), (2, 0), (2, 1), (1, 2), (2, -1), (-1, 2))
BLOCKS = 4


def remote(src, dst, send, recv, **device):
    return pltpu.make_async_remote_copy(src_ref=src, dst_ref=dst, send_sem=send, recv_sem=recv, device_id=device, device_id_type=MESH)


def moe_kernel(n_rank, n_loc, capacity, x_hbm, wg, wu, wd, ids, gate_vals, out, wfull, yret, tok, meta, slots_send, slots_own, gates_own, rows_in, wbuf, ybuf, retbuf, acc, ring_s, ring_r, part_s, part_r, fine_s, fine_r, fpart_s, fpart_r, line_s, line_r, plane_s, plane_r, meta_s, meta_r, y_s, y_r, yb_s, yb_r, load_sem, own_sem, ownb_sem, ret_sem, retb_sem, tok_sem):
    ep = lax.axis_index("ep")
    tp = lax.axis_index("tp")
    z, y = ep // RING, lax.rem(ep, RING)
    x, core = tp // CORES, lax.rem(tp, CORES)
    weights = (wg, wu, wd)
    cols = wg.shape[1]
    half = cols // 2
    tok_loc = x_hbm.shape[0]
    quart = tok_loc // 4
    n_rows = n_rank * capacity

    def step(pos, amount):
        return lax.rem(pos + amount + 2 * RING, RING)

    ring_to = (step(x, 1) * CORES + core, step(x, -1) * CORES + core)
    partner = x * CORES + 1 - core

    def chunk_rows(t, d):
        return pl.ds(pl.multiple_of(t * cols + d * half, 16), half)

    def ring_in_x(d, s):
        return step(x, -1 - s) if d == 0 else step(x, 1 + s)

    def ring_start(d, s, e):
        if s == 0:
            rows = chunk_rows(tp, d)
            for i, w in enumerate(weights):
                remote(w.at[e, pl.ds(d * half, half), :], wfull.at[e, i, rows, :], ring_s.at[d, s, e], ring_r.at[d, s, e], tp=ring_to[d]).start()
        else:
            piece = wfull.at[e, :, chunk_rows(ring_in_x(d, s - 1) * CORES + core, d), :]
            remote(piece, piece, ring_s.at[d, s, e], ring_r.at[d, s, e], tp=ring_to[d]).start()

    def ring_desc(d, s, e):
        piece = wfull.at[e, :, chunk_rows(ring_in_x(d, s) * CORES + core, d), :]
        return remote(piece, piece, ring_s.at[d, s, e], ring_r.at[d, s, e], tp=ring_to[d])

    def own_rows(t):
        return pl.ds(pl.multiple_of(t * cols, 16), cols)

    def share_own(e):
        for i, w in enumerate(weights):
            remote(w.at[e], wfull.at[e, i, own_rows(tp), :], part_s.at[6, e], part_r.at[6, e], tp=partner).start()

    def share_own_desc(e):
        piece = wfull.at[e, :, own_rows(partner), :]
        return remote(piece, piece, part_s.at[6, e], part_r.at[6, e], tp=partner)

    def share(d, s, e):
        piece = wfull.at[e, :, chunk_rows(ring_in_x(d, s) * CORES + core, d), :]
        remote(piece, piece, part_s.at[d * 3 + s, e], part_r.at[d * 3 + s, e], tp=partner).start()

    def share_desc(d, s, e):
        piece = wfull.at[e, :, chunk_rows(ring_in_x(d, s) * CORES + 1 - core, d), :]
        return remote(piece, piece, part_s.at[d * 3 + s, e], part_r.at[d * 3 + s, e], tp=partner)

    coarse = n_loc - 2
    width = x_hbm.shape[1] // BLOCKS
    parts6 = (0, 1, 2)
    parts7 = (3, 4)
    down7 = tuple(range(5, 5 + BLOCKS))

    def fine_at(q):
        if q < 3:
            return coarse, q, slice(None)
        if q < 5:
            return coarse + 1, q - 3, slice(None)
        return coarse + 1, 2, pl.ds((q - 5) * width, width)

    def fine_own(q, rows):
        e, i, c = fine_at(q)
        return weights[i].at[e, rows, c]

    def fine_land(q, rows):
        e, i, c = fine_at(q)
        return wfull.at[e, i, rows, c]

    def fine_start(d, s, q):
        if s == 0:
            src, dst = fine_own(q, pl.ds(d * half, half)), fine_land(q, chunk_rows(tp, d))
        else:
            src = dst = fine_land(q, chunk_rows(ring_in_x(d, s - 1) * CORES + core, d))
        remote(src, dst, fine_s.at[d, s, q], fine_r.at[d, s, q], tp=ring_to[d]).start()

    def fine_desc(d, s, q):
        piece = fine_land(q, chunk_rows(ring_in_x(d, s) * CORES + core, d))
        return remote(piece, piece, fine_s.at[d, s, q], fine_r.at[d, s, q], tp=ring_to[d])

    def fine_share_own(q):
        remote(fine_own(q, pl.ds(0, cols)), fine_land(q, own_rows(tp)), fpart_s.at[6, q], fpart_r.at[6, q], tp=partner).start()

    def fine_share_own_desc(q):
        piece = fine_land(q, own_rows(partner))
        return remote(piece, piece, fpart_s.at[6, q], fpart_r.at[6, q], tp=partner)

    def fine_share(d, s, q):
        piece = fine_land(q, chunk_rows(ring_in_x(d, s) * CORES + core, d))
        remote(piece, piece, fpart_s.at[d * 3 + s, q], fpart_r.at[d * 3 + s, q], tp=partner).start()

    def fine_share_desc(d, s, q):
        piece = fine_land(q, chunk_rows(ring_in_x(d, s) * CORES + 1 - core, d))
        return remote(piece, piece, fpart_s.at[d * 3 + s, q], fpart_r.at[d * 3 + s, q], tp=partner)

    def fine_forward(s, items):
        for q in items:
            for d in range(2):
                fine_desc(d, s, q).wait_recv()
                if s < 2:
                    fine_start(d, s + 1, q)
                else:
                    fine_share(d, s, q)

    def fine_share_all(s, items):
        for q in items:
            for d in range(2):
                fine_share(d, s, q)

    def fine_load(q):
        fine_share_own_desc(q).wait_recv()
        for d in range(2):
            for s in range(3):
                fine_share_desc(d, s, q).wait_recv()
        e, i, c = fine_at(q)
        copies = [pltpu.make_async_copy(fine_own(q, pl.ds(0, cols)), wbuf.at[i, own_rows(tp), c], load_sem.at[q, 0])]
        for j in range(1, RING * CORES):
            other = own_rows(lax.rem(tp + j, RING * CORES))
            copies.append(pltpu.make_async_copy(fine_land(q, other), wbuf.at[i, other, c], load_sem.at[q, j]))
        for c in copies:
            c.start()
        return copies

    routes = (("y", 1), ("y", -1), ("z", 1), ("z", -1))

    def plane_peer(axis, amount):
        return z * RING + step(y, amount) if axis == "y" else step(z, amount) * RING + y

    def quarter(q):
        return pl.ds(q * quart, quart)

    def line_piece(q, back):
        axis, sign = routes[q]
        if axis == "y":
            return tok.at[z, step(y, -sign * back), quarter(q), :]
        return tok.at[step(z, -sign * back), y, quarter(q), :]

    def line_start(q, s):
        axis, sign = routes[q]
        src = x_hbm.at[quarter(q), :] if s == 0 else line_piece(q, s)
        remote(src, line_piece(q, s), line_s.at[q, s], line_r.at[q, s], ep=plane_peer(axis, sign)).start()

    def line_desc(q, s):
        axis, sign = routes[q]
        piece = line_piece(q, s + 1)
        return remote(piece, piece, line_s.at[q, s], line_r.at[q, s], ep=plane_peer(axis, sign))

    def plane_piece(q, back):
        axis, sign = routes[q]
        if axis == "y":
            return tok.at[step(z, -sign * back), :, quarter(q), :]
        return tok.at[:, step(y, -sign * back), quarter(q), :]

    def plane_start(q, s):
        axis, sign = routes[q]
        piece = plane_piece(q, s)
        remote(piece, piece, plane_s.at[q, s], plane_r.at[q, s], ep=plane_peer("z" if axis == "y" else "y", sign)).start()

    def plane_desc(q, s):
        axis, sign = routes[q]
        piece = plane_piece(q, s + 1)
        return remote(piece, piece, plane_s.at[q, s], plane_r.at[q, s], ep=plane_peer("z" if axis == "y" else "y", sign))

    def peer(j):
        dz, dy = ROUND[j - 1]
        return step(z, dz) * RING + step(y, dy)

    def back_peer(j):
        dz, dy = ROUND[j - 1]
        return step(z, -dz) * RING + step(y, -dy)

    def src_rows(r):
        return pl.ds(pl.multiple_of(r * capacity, capacity), capacity)

    def y_send(e, k, j):
        r = peer(j)
        return remote(ybuf.at[k, src_rows(r), :], yret.at[e, ep], y_s.at[k, j], y_r.at[e, j], ep=r)

    def y_recv(e, j):
        r = back_peer(j)
        return remote(yret.at[e, r], yret.at[e, r], y_s.at[0, j], y_r.at[e, j], ep=peer(j))

    def y_own(e, k):
        return pltpu.make_async_copy(ybuf.at[k, src_rows(ep), :], yret.at[e, ep], own_sem.at[k])

    def yb_send(n, j):
        r, c = peer(j), pl.ds(n * width, width)
        return remote(ybuf.at[1, src_rows(r), c], yret.at[n_loc - 1, ep, :, c], yb_s.at[n, j], yb_r.at[n, j], ep=r)

    def yb_recv(n, j):
        r, c = back_peer(j), pl.ds(n * width, width)
        piece = yret.at[n_loc - 1, r, :, c]
        return remote(piece, piece, yb_s.at[n, j], yb_r.at[n, j], ep=peer(j))

    def yb_own(n):
        c = pl.ds(n * width, width)
        return pltpu.make_async_copy(ybuf.at[1, src_rows(ep), c], yret.at[n_loc - 1, ep, :, c], ownb_sem.at[n])

    barrier = pltpu.get_barrier_semaphore()
    for j in range(1, n_rank):
        pl.semaphore_signal(barrier, inc=1, device_id={"ep": peer(j)}, device_id_type=MESH)
    for t in (*ring_to, partner):
        pl.semaphore_signal(barrier, inc=1, device_id={"tp": t}, device_id_type=MESH)
    pl.semaphore_wait(barrier, n_rank - 1 + 3)

    def ring_issue(b, static):
        def when(cond, fn):
            if static:
                if cond:
                    fn()
            else:
                pl.when(cond)(fn)

        def first():
            for d in range(2):
                ring_desc(d, 0, b).wait_recv()
                ring_start(d, 1, b)
            for d in range(2):
                share(d, 0, b)

        def second():
            for d in range(2):
                ring_desc(d, 1, b - 1).wait_recv()
                ring_start(d, 2, b - 1)
            for d in range(2):
                share(d, 1, b - 1)

        def ahead():
            for d in range(2):
                ring_start(d, 0, b + 2)
            share_own(b + 2)

        def ahead_fine():
            for q in parts6:
                for d in range(2):
                    fine_start(d, 0, q)
            for q in parts6:
                fine_share_own(q)

        first()
        if static:
            if 1 <= b:
                second()
        else:
            second()
        when(b + 2 < coarse, ahead)
        when(b + 2 == coarse, ahead_fine)

    def mix_parts(e):
        slot_iota = lax.broadcasted_iota(jnp.int32, (n_rank, capacity, tok_loc), 1).astype(F32)
        place = slots_own[e][:, None, :] == slot_iota
        mix = jnp.where(place, gates_own[e][:, None, :], 0.0).reshape(n_rows, tok_loc).T
        hi = mix.astype(BF16)
        rest = mix - hi.astype(F32)
        mid = rest.astype(BF16)
        low = (rest - mid.astype(F32)).astype(BF16)
        return hi, mid, low

    def mixed(parts, ret):
        ret = ret.reshape(n_rows, width)
        hi, mid, low = (jnp.dot(p, ret, preferred_element_type=F32) for p in parts)
        return hi + mid + low

    def combine(e):
        for j in range(1, n_rank):
            y_recv(e, j).wait_recv()
        y_own(e, e % 2 if isinstance(e, int) else lax.rem(e, 2)).wait()
        load = pltpu.make_async_copy(yret.at[e], retbuf, ret_sem)
        load.start()
        parts = mix_parts(e)
        load.wait()
        for n in range(BLOCKS):
            blk = pl.ds(n * width, width)
            acc[:, blk] += mixed(parts, retbuf[:, :, blk])

    def hidden_of(e):
        xe = rows_in[e]
        hidden = []
        for f in range(3):
            blk = pl.ds(f * 256, 256)
            dims = (((1,), (1,)), ((), ()))
            a = lax.dot_general(xe, wbuf[0, blk, :], dims, preferred_element_type=F32)
            b = lax.dot_general(xe, wbuf[1, blk, :], dims, preferred_element_type=F32)
            hidden.append((jax.nn.silu(a) * b).astype(BF16))
        return jnp.concatenate(hidden, axis=1)

    def down(h, k, n):
        blk = pl.ds(n * width, width)
        ybuf[k, :, blk] = jnp.dot(h, wbuf[2, :, blk], preferred_element_type=F32).astype(BF16)

    def expert(e):
        for d in range(2):
            ring_desc(d, 2, e).wait_recv()
            share(d, 2, e)
        share_own_desc(e).wait_recv()
        for d in range(2):
            for s in range(3):
                share_desc(d, s, e).wait_recv()
        copies = []
        for i, w in enumerate(weights):
            copies.append(pltpu.make_async_copy(w.at[e], wbuf.at[i, own_rows(tp), :], load_sem.at[0, i]))
        for j in range(1, RING * CORES):
            other = own_rows(lax.rem(tp + j, RING * CORES))
            copies.append(pltpu.make_async_copy(wfull.at[e, :, other, :], wbuf.at[:, other, :], load_sem.at[1, j]))
        for c in copies:
            c.start()
        k = e % 2 if isinstance(e, int) else lax.rem(e, 2)

        def free_slot():
            for j in range(1, n_rank):
                y_send(e - 2, k, j).wait_send()

        if isinstance(e, int):
            free_slot()
        else:
            pl.when(e >= 2)(free_slot)

        for c in copies:
            c.wait()
        h = hidden_of(e)
        for n in range(BLOCKS):
            down(h, k, n)
        y_own(e, k).start()
        for j in range(1, n_rank):
            y_send(e, k, j).start()

    for b in range(2):
        for d in range(2):
            ring_start(d, 0, b)
    for q in range(4):
        line_start(q, 0)
    load_own = pltpu.make_async_copy(x_hbm, tok.at[z, y], tok_sem)
    load_own.start()
    for b in range(2):
        share_own(b)

    n_exp = n_rank * n_loc
    row = lax.broadcasted_iota(jnp.int32, (n_exp, tok_loc), 0)
    square = (tok_loc, tok_loc)
    before = jnp.where(lax.broadcasted_iota(jnp.int32, square, 0) < lax.broadcasted_iota(jnp.int32, square, 1), 1.0, 0.0).astype(BF16)

    def slot_map(expert_of_row):
        chosen = jnp.zeros((n_exp, tok_loc), F32)
        gates = jnp.zeros((n_exp, tok_loc), F32)
        for j in range(ids.shape[0]):
            hit = ids[j:j + 1, :] == expert_of_row
            chosen = jnp.where(hit, 1.0, chosen)
            gates = jnp.where(hit, gate_vals[j:j + 1, :], gates)
        slots = jnp.dot(chosen.astype(BF16), before, preferred_element_type=F32)
        return jnp.where((chosen > 0.5) & (slots < capacity - 0.5), slots, -1.0), gates

    slots_send[...] = slot_map(row)[0].reshape(slots_send.shape)
    slots, gates = slot_map(lax.rem(row, n_rank) * n_loc + row // n_rank)
    slots_own[...] = slots.reshape(slots_own.shape)
    gates_own[...] = gates.reshape(gates_own.shape)
    acc[...] = jnp.zeros_like(acc)
    for s in range(2):
        for q in range(4):
            line_desc(q, s).wait_recv()
            line_start(q, s + 1)
        if s == 0:
            for j in range(1, n_rank):
                remote(slots_send.at[peer(j)], meta.at[ep], meta_s.at[j], meta_r.at[j], ep=peer(j)).start()
            meta[ep] = slots_send[ep]
    ring_issue(0, True)
    load_own.wait()
    for q in range(4):
        line_desc(q, 2).wait_recv()
    for q in range(4):
        plane_start(q, 0)
    ring_issue(1, True)
    for q in range(4):
        plane_desc(q, 0).wait_recv()
        plane_start(q, 1)
    ring_issue(2, True)
    for q in range(4):
        plane_desc(q, 1).wait_recv()
        plane_start(q, 2)
    for q in range(4):
        plane_desc(q, 2).wait_recv()
    for j in range(1, n_rank):
        remote(slots_send.at[back_peer(j)], meta.at[back_peer(j)], meta_s.at[j], meta_r.at[j], ep=peer(j)).wait_recv()

    @pl.loop(0, n_rank)
    def _(s):
        slot_iota = lax.broadcasted_iota(jnp.int32, (n_loc, capacity, tok_loc), 1).astype(F32)
        pick = jnp.where(meta[s][:, None, :] == slot_iota, 1.0, 0.0).reshape(n_loc * capacity, tok_loc).astype(BF16)
        picked = jnp.dot(pick, tok[s // RING, lax.rem(s, RING)], preferred_element_type=F32).astype(BF16)
        for e in range(n_loc):
            rows_in[e, src_rows(s), :] = picked[e * capacity:(e + 1) * capacity]

    @pl.loop(2, coarse)
    def _(b):
        @pl.when(b > 2)
        def _():
            ring_issue(b, False)

        expert(b - 2)

        @pl.when(b > 2)
        def _():
            combine(b - 3)

    for d in range(2):
        ring_desc(d, 1, coarse - 1).wait_recv()
        ring_start(d, 2, coarse - 1)
        share(d, 1, coarse - 1)
    fine_forward(0, parts6)
    fine_share_all(0, parts6)
    expert(coarse - 2)
    combine(coarse - 3)
    expert(coarse - 1)
    fine_forward(1, parts6)
    for q in parts7 + down7:
        for d in range(2):
            fine_start(d, 0, q)
    fine_share_all(1, parts6)
    for q in parts7 + down7:
        fine_share_own(q)
    combine(coarse - 2)

    fine_forward(2, parts6)
    loads = fine_load(0) + fine_load(1)
    for c in loads:
        c.wait()
    loads = fine_load(2)
    h = hidden_of(coarse)
    fine_forward(0, parts7)
    fine_share_all(0, parts7)
    for j in range(1, n_rank):
        y_send(coarse - 2, 0, j).wait_send()
    for c in loads:
        c.wait()
    for n in range(BLOCKS):
        down(h, 0, n)
    y_own(coarse, 0).start()
    for j in range(1, n_rank):
        y_send(coarse, 0, j).start()

    fine_forward(1, parts7)
    fine_forward(0, down7)
    fine_share_all(1, parts7)
    fine_share_all(0, down7)
    combine(coarse - 1)
    fine_forward(2, parts7)
    fine_forward(1, down7)
    fine_share_all(1, down7)
    loads = fine_load(3) + fine_load(4)
    for c in loads:
        c.wait()
    h = hidden_of(coarse + 1)
    for j in range(1, n_rank):
        y_send(coarse - 1, 1, j).wait_send()
    fine_forward(2, down7)
    block_loads = [fine_load(q) for q in down7]
    for n in range(BLOCKS):
        for c in block_loads[n]:
            c.wait()
        down(h, 1, n)
        yb_own(n).start()
        for j in range(1, n_rank):
            yb_send(n, j).start()
    combine(coarse)
    parts = mix_parts(coarse + 1)
    for n in range(BLOCKS):
        blk = pl.ds(n * width, width)
        for j in range(1, n_rank):
            yb_recv(n, j).wait_recv()
        yb_own(n).wait()
        load = pltpu.make_async_copy(yret.at[coarse + 1, :, :, blk], retbuf.at[:, :, blk], retb_sem.at[n])
        load.start()
        load.wait()
        out[:, blk] = (acc[:, blk] + mixed(parts, retbuf[:, :, blk])).astype(out.dtype)

    for j in range(1, n_rank):
        y_send(coarse, 0, j).wait_send()
        for n in range(BLOCKS):
            yb_send(n, j).wait_send()
    for q in range(5 + BLOCKS):
        fine_share_own_desc(q).wait_send()
        for d in range(2):
            for s in range(3):
                fine_desc(d, s, q).wait_send()
                fine_share_desc(d, s, q).wait_send()
    for q in range(4):
        for s in range(3):
            line_desc(q, s).wait_send()
            plane_desc(q, s).wait_send()
    for j in range(1, n_rank):
        remote(slots_send.at[peer(j)], meta.at[ep], meta_s.at[j], meta_r.at[j], ep=peer(j)).wait_send()

    @pl.loop(0, coarse)
    def _(e):
        share_own_desc(e).wait_send()
        for d in range(2):
            for s in range(3):
                ring_desc(d, s, e).wait_send()
                share_desc(d, s, e).wait_send()


def solution(mesh):
    expert_ranks = mesh.shape["ep"]
    row_spec = P(("dp", "ep", "tp"), None)

    def local_layer(x_loc, ids_loc, gate_loc, wg_loc, wu_loc, wd_loc):
        tok_loc, d_model = x_loc.shape
        n_top = ids_loc.shape[1]
        local_exp, _, cols = wg_loc.shape
        ffn = cols * mesh.shape["tp"]
        n_exp = local_exp * expert_ranks
        capacity = CAP_FACTOR * n_top * tok_loc // n_exp
        n_rows = expert_ranks * capacity
        any_spec = pl.BlockSpec(memory_space=pl.ANY)
        vmem_spec = pl.BlockSpec(memory_space=pltpu.VMEM)
        dma = pltpu.SemaphoreType.DMA
        out = pl.pallas_call(
            functools.partial(moe_kernel, expert_ranks, local_exp, capacity),
            out_shape=(
                jax.ShapeDtypeStruct((tok_loc, d_model), BF16),
                jax.ShapeDtypeStruct((local_exp, 3, ffn, d_model), BF16),
                jax.ShapeDtypeStruct((local_exp, expert_ranks, capacity, d_model), BF16),
            ),
            in_specs=[any_spec] * 4 + [vmem_spec] * 2,
            out_specs=(vmem_spec, any_spec, any_spec),
            scratch_shapes=[
                pltpu.VMEM((RING, RING, tok_loc, d_model), BF16),
                pltpu.VMEM((expert_ranks, local_exp, tok_loc), F32),
                pltpu.VMEM((expert_ranks, local_exp, tok_loc), F32),
                pltpu.VMEM((local_exp, expert_ranks, tok_loc), F32),
                pltpu.VMEM((local_exp, expert_ranks, tok_loc), F32),
                pltpu.VMEM((local_exp, n_rows, d_model), BF16),
                pltpu.VMEM((3, ffn, d_model), BF16),
                pltpu.VMEM((2, n_rows, d_model), BF16),
                pltpu.VMEM((expert_ranks, capacity, d_model), BF16),
                pltpu.VMEM((tok_loc, d_model), F32),
                dma((2, 3, local_exp - 2)),
                dma((2, 3, local_exp - 2)),
                dma((7, local_exp - 2)),
                dma((7, local_exp - 2)),
                dma((2, 3, 5 + BLOCKS)),
                dma((2, 3, 5 + BLOCKS)),
                dma((7, 5 + BLOCKS)),
                dma((7, 5 + BLOCKS)),
                dma((4, 3)),
                dma((4, 3)),
                dma((4, 3)),
                dma((4, 3)),
                dma((expert_ranks,)),
                dma((expert_ranks,)),
                dma((2, expert_ranks)),
                dma((local_exp, expert_ranks)),
                dma((BLOCKS, expert_ranks)),
                dma((BLOCKS, expert_ranks)),
                dma((5 + BLOCKS, 8)),
                dma((2,)),
                dma((BLOCKS,)),
                dma,
                dma((BLOCKS,)),
                dma,
            ],
            compiler_params=pltpu.CompilerParams(collective_id=0, has_side_effects=True, vmem_limit_bytes=67000000),
        )(
            x_loc,
            jnp.swapaxes(wg_loc, 1, 2),
            jnp.swapaxes(wu_loc, 1, 2),
            wd_loc,
            ids_loc.T,
            gate_loc.T,
        )
        return out[0]

    return jax.shard_map(local_layer, mesh=mesh, in_specs=(row_spec, row_spec, row_spec, P("ep", None, "tp"), P("ep", None, "tp"), P("ep", "tp", None)), out_specs=row_spec, check_vma=False)
```

```python
import functools

import jax
import jax.numpy as jnp
from jax import lax
from jax.experimental import pallas as pl
from jax.experimental.pallas import tpu as pltpu
from jax.sharding import PartitionSpec as P

CAP_FACTOR = 2
RING = 4
CORES = 2
MESH = pl.DeviceIdType.MESH
F32 = jnp.float32
BF16 = jnp.bfloat16


ROUND = ((0, 1), (0, -1), (1, 0), (-1, 0), (2, 2), (1, 1), (-1, -1), (1, -1), (-1, 1), (0, 2), (2, 0), (2, 1), (1, 2), (2, -1), (-1, 2))
BLOCKS = 4


def remote(src, dst, send, recv, **device):
    return pltpu.make_async_remote_copy(src_ref=src, dst_ref=dst, send_sem=send, recv_sem=recv, device_id=device, device_id_type=MESH)


def moe_kernel(n_rank, n_loc, capacity, x_hbm, wg, wu, wd, ids, gate_vals, out, wfull, yret, tok, meta, slots_send, slots_own, gates_own, rows_in, wbuf, wlast, ybuf, retbuf, retlast, hid, acc, ring_s, ring_r, part_s, part_r, fine_s, fine_r, fpart_s, fpart_r, line_s, line_r, plane_s, plane_r, meta_s, meta_r, y_s, y_r, yb_s, yb_r, load_sem, last_sem, own_sem, ret_sem, out_sem, tok_sem):
    ep = lax.axis_index("ep")
    tp = lax.axis_index("tp")
    z, y = ep // RING, lax.rem(ep, RING)
    x, core = tp // CORES, lax.rem(tp, CORES)
    weights = (wg, wu, wd)
    cols = wg.shape[1]
    half = cols // 2
    tok_loc = x_hbm.shape[0]
    quart = tok_loc // 4
    n_rows = n_rank * capacity

    def step(pos, amount):
        return lax.rem(pos + amount + 2 * RING, RING)

    ring_to = (step(x, 1) * CORES + core, step(x, -1) * CORES + core)
    partner = x * CORES + 1 - core

    def chunk_rows(t, d):
        return pl.ds(pl.multiple_of(t * cols + d * half, 16), half)

    def ring_in_x(d, s):
        return step(x, -1 - s) if d == 0 else step(x, 1 + s)

    def ring_start(d, s, e):
        if s == 0:
            rows = chunk_rows(tp, d)
            for i, w in enumerate(weights):
                remote(w.at[e, pl.ds(d * half, half), :], wfull.at[e, i, rows, :], ring_s.at[d, s, e], ring_r.at[d, s, e], tp=ring_to[d]).start()
        else:
            piece = wfull.at[e, :, chunk_rows(ring_in_x(d, s - 1) * CORES + core, d), :]
            remote(piece, piece, ring_s.at[d, s, e], ring_r.at[d, s, e], tp=ring_to[d]).start()

    def ring_desc(d, s, e):
        piece = wfull.at[e, :, chunk_rows(ring_in_x(d, s) * CORES + core, d), :]
        return remote(piece, piece, ring_s.at[d, s, e], ring_r.at[d, s, e], tp=ring_to[d])

    def own_rows(t):
        return pl.ds(pl.multiple_of(t * cols, 16), cols)

    def share_own(e):
        for i, w in enumerate(weights):
            remote(w.at[e], wfull.at[e, i, own_rows(tp), :], part_s.at[6, e], part_r.at[6, e], tp=partner).start()

    def share_own_desc(e):
        piece = wfull.at[e, :, own_rows(partner), :]
        return remote(piece, piece, part_s.at[6, e], part_r.at[6, e], tp=partner)

    def share(d, s, e):
        piece = wfull.at[e, :, chunk_rows(ring_in_x(d, s) * CORES + core, d), :]
        remote(piece, piece, part_s.at[d * 3 + s, e], part_r.at[d * 3 + s, e], tp=partner).start()

    def share_desc(d, s, e):
        piece = wfull.at[e, :, chunk_rows(ring_in_x(d, s) * CORES + 1 - core, d), :]
        return remote(piece, piece, part_s.at[d * 3 + s, e], part_r.at[d * 3 + s, e], tp=partner)

    coarse = n_loc - 2
    width = x_hbm.shape[1] // BLOCKS
    third = wbuf.shape[1] // 3
    parts6 = (0, 1, 2)
    parts7 = (3, 4)
    down7 = tuple(range(5, 5 + BLOCKS))

    def fine_at(q):
        if q < 3:
            return coarse, q, slice(None)
        if q < 5:
            return coarse + 1, q - 3, slice(None)
        return coarse + 1, 2, pl.ds((q - 5) * width, width)

    def fine_own(q, rows):
        e, i, c = fine_at(q)
        return weights[i].at[e, rows, c]

    def fine_land(q, rows):
        e, i, c = fine_at(q)
        return wfull.at[e, i, rows, c] if q < 3 else wlast.at[i, rows, c]

    def fine_start(d, s, q):
        if s == 0:
            src, dst = fine_own(q, pl.ds(d * half, half)), fine_land(q, chunk_rows(tp, d))
        else:
            src = dst = fine_land(q, chunk_rows(ring_in_x(d, s - 1) * CORES + core, d))
        remote(src, dst, fine_s.at[d, s, q], fine_r.at[d, s, q], tp=ring_to[d]).start()

    def fine_desc(d, s, q):
        piece = fine_land(q, chunk_rows(ring_in_x(d, s) * CORES + core, d))
        return remote(piece, piece, fine_s.at[d, s, q], fine_r.at[d, s, q], tp=ring_to[d])

    def fine_share_own(q):
        remote(fine_own(q, pl.ds(0, cols)), fine_land(q, own_rows(tp)), fpart_s.at[6, q], fpart_r.at[6, q], tp=partner).start()

    def fine_share_own_desc(q):
        piece = fine_land(q, own_rows(partner))
        return remote(piece, piece, fpart_s.at[6, q], fpart_r.at[6, q], tp=partner)

    def fine_share(d, s, q):
        piece = fine_land(q, chunk_rows(ring_in_x(d, s) * CORES + core, d))
        remote(piece, piece, fpart_s.at[d * 3 + s, q], fpart_r.at[d * 3 + s, q], tp=partner).start()

    def fine_share_desc(d, s, q):
        piece = fine_land(q, chunk_rows(ring_in_x(d, s) * CORES + 1 - core, d))
        return remote(piece, piece, fpart_s.at[d * 3 + s, q], fpart_r.at[d * 3 + s, q], tp=partner)

    def fine_forward(s, items):
        for q in items:
            for d in range(2):
                fine_desc(d, s, q).wait_recv()
                if s < 2:
                    fine_start(d, s + 1, q)
                else:
                    fine_share(d, s, q)

    def fine_share_all(s, items):
        for q in items:
            for d in range(2):
                fine_share(d, s, q)

    def fine_shared(q):
        fine_share_own_desc(q).wait_recv()
        for d in range(2):
            for s in range(3):
                fine_share_desc(d, s, q).wait_recv()

    def last_own(i):
        return pltpu.make_async_copy(weights[i].at[coarse + 1], wlast.at[i, own_rows(tp), :], last_sem.at[i])

    def fine_load(q):
        fine_shared(q)
        e, i, c = fine_at(q)
        copies = [pltpu.make_async_copy(fine_own(q, pl.ds(0, cols)), wbuf.at[i, own_rows(tp), c], load_sem.at[q, 0])]
        for j in range(1, RING * CORES):
            other = own_rows(lax.rem(tp + j, RING * CORES))
            copies.append(pltpu.make_async_copy(fine_land(q, other), wbuf.at[i, other, c], load_sem.at[q, j]))
        for c in copies:
            c.start()
        return copies

    routes = (("y", 1), ("y", -1), ("z", 1), ("z", -1))

    def plane_peer(axis, amount):
        return z * RING + step(y, amount) if axis == "y" else step(z, amount) * RING + y

    def quarter(q):
        return pl.ds(q * quart, quart)

    def line_piece(q, back):
        axis, sign = routes[q]
        if axis == "y":
            return tok.at[z, step(y, -sign * back), quarter(q), :]
        return tok.at[step(z, -sign * back), y, quarter(q), :]

    def line_start(q, s):
        axis, sign = routes[q]
        src = x_hbm.at[quarter(q), :] if s == 0 else line_piece(q, s)
        remote(src, line_piece(q, s), line_s.at[q, s], line_r.at[q, s], ep=plane_peer(axis, sign)).start()

    def line_desc(q, s):
        axis, sign = routes[q]
        piece = line_piece(q, s + 1)
        return remote(piece, piece, line_s.at[q, s], line_r.at[q, s], ep=plane_peer(axis, sign))

    def plane_piece(q, back):
        axis, sign = routes[q]
        if axis == "y":
            return tok.at[step(z, -sign * back), :, quarter(q), :]
        return tok.at[:, step(y, -sign * back), quarter(q), :]

    def plane_start(q, s):
        axis, sign = routes[q]
        piece = plane_piece(q, s)
        remote(piece, piece, plane_s.at[q, s], plane_r.at[q, s], ep=plane_peer("z" if axis == "y" else "y", sign)).start()

    def plane_desc(q, s):
        axis, sign = routes[q]
        piece = plane_piece(q, s + 1)
        return remote(piece, piece, plane_s.at[q, s], plane_r.at[q, s], ep=plane_peer("z" if axis == "y" else "y", sign))

    def peer(j):
        dz, dy = ROUND[j - 1]
        return step(z, dz) * RING + step(y, dy)

    def back_peer(j):
        dz, dy = ROUND[j - 1]
        return step(z, -dz) * RING + step(y, -dy)

    def src_rows(r):
        return pl.ds(pl.multiple_of(r * capacity, capacity), capacity)

    def y_send(e, k, j):
        r = peer(j)
        return remote(ybuf.at[k, src_rows(r), :], yret.at[e, ep], y_s.at[k, j], y_r.at[e, j], ep=r)

    def y_recv(e, j):
        r = back_peer(j)
        return remote(yret.at[e, r], yret.at[e, r], y_s.at[0, j], y_r.at[e, j], ep=peer(j))

    def y_own(e, k):
        return pltpu.make_async_copy(ybuf.at[k, src_rows(ep), :], yret.at[e, ep], own_sem.at[k])

    def yb_send(n, j):
        r, c = peer(j), pl.ds(n * width, width)
        return remote(ybuf.at[1, src_rows(r), c], retlast.at[ep, :, c], yb_s.at[n, j], yb_r.at[n, j], ep=r)

    def yb_recv(n, j):
        r, c = back_peer(j), pl.ds(n * width, width)
        piece = retlast.at[r, :, c]
        return remote(piece, piece, yb_s.at[n, j], yb_r.at[n, j], ep=peer(j))

    barrier = pltpu.get_barrier_semaphore()
    for j in range(1, n_rank):
        pl.semaphore_signal(barrier, inc=1, device_id={"ep": peer(j)}, device_id_type=MESH)
    for t in (*ring_to, partner):
        pl.semaphore_signal(barrier, inc=1, device_id={"tp": t}, device_id_type=MESH)
    pl.semaphore_wait(barrier, n_rank - 1 + 3)

    def send_first(e):
        for d in range(2):
            ring_start(d, 0, e)
        share_own(e)

    def forward(s, e):
        for d in range(2):
            ring_desc(d, s, e).wait_recv()
            ring_start(d, s + 1, e)
        for d in range(2):
            share(d, s, e)

    def fine_first(items):
        for q in items:
            for d in range(2):
                fine_start(d, 0, q)
        for q in items:
            fine_share_own(q)

    def mix_parts(e):
        slot_iota = lax.broadcasted_iota(jnp.int32, (n_rank, capacity, tok_loc), 1).astype(F32)
        place = slots_own[e][:, None, :] == slot_iota
        mix = jnp.where(place, gates_own[e][:, None, :], 0.0).reshape(n_rows, tok_loc).T
        hi = mix.astype(BF16)
        rest = mix - hi.astype(F32)
        mid = rest.astype(BF16)
        low = (rest - mid.astype(F32)).astype(BF16)
        return hi, mid, low

    def mixed(parts, ret):
        ret = ret.reshape(n_rows, width)
        hi, mid, low = (jnp.dot(p, ret, preferred_element_type=F32) for p in parts)
        return hi + mid + low

    def combine(e):
        for j in range(1, n_rank):
            y_recv(e, j).wait_recv()
        y_own(e, e % 2 if isinstance(e, int) else lax.rem(e, 2)).wait()
        load = pltpu.make_async_copy(yret.at[e], retbuf, ret_sem)
        load.start()
        parts = mix_parts(e)
        load.wait()
        for n in range(BLOCKS):
            blk = pl.ds(n * width, width)
            acc[:, blk] += mixed(parts, retbuf[:, :, blk])

    def hidden_third(e, w, f):
        blk = pl.ds(pl.multiple_of(f * third, third) if not isinstance(f, int) else f * third, third)
        dims = (((1,), (1,)), ((), ()))
        xe = rows_in[e]
        a = lax.dot_general(xe, w[0, blk, :], dims, preferred_element_type=F32)
        b = lax.dot_general(xe, w[1, blk, :], dims, preferred_element_type=F32)
        hid[:, blk] = (jax.nn.silu(a) * b).astype(BF16)

    def hidden_of(e, w):
        @pl.loop(0, 3)
        def _(f):
            hidden_third(e, w, f)

    def down(k, w, n):
        blk = pl.ds(pl.multiple_of(n * width, width) if not isinstance(n, int) else n * width, width)
        ybuf[k, :, blk] = jnp.dot(hid[...], w[2, :, blk], preferred_element_type=F32).astype(BF16)

    def down_all(k, w):
        @pl.loop(0, BLOCKS)
        def _(n):
            down(k, w, n)

    def expert(e):
        for d in range(2):
            ring_desc(d, 2, e).wait_recv()
            share(d, 2, e)
        share_own_desc(e).wait_recv()
        for d in range(2):
            for s in range(3):
                share_desc(d, s, e).wait_recv()
        copies = []
        for i, w in enumerate(weights):
            copies.append(pltpu.make_async_copy(w.at[e], wbuf.at[i, own_rows(tp), :], load_sem.at[0, i]))
        for j in range(1, RING * CORES):
            other = own_rows(lax.rem(tp + j, RING * CORES))
            copies.append(pltpu.make_async_copy(wfull.at[e, :, other, :], wbuf.at[:, other, :], load_sem.at[1, j]))
        for c in copies:
            c.start()
        k = e % 2 if isinstance(e, int) else lax.rem(e, 2)

        def free_slot():
            for j in range(1, n_rank):
                y_send(e - 2, k, j).wait_send()

        if isinstance(e, int):
            free_slot()
        else:
            pl.when(e >= 2)(free_slot)

        for c in copies:
            c.wait()
        hidden_of(e, wbuf)
        down_all(k, wbuf)
        y_own(e, k).start()
        for j in range(1, n_rank):
            y_send(e, k, j).start()

    for b in range(2):
        for d in range(2):
            ring_start(d, 0, b)
    for q in range(4):
        line_start(q, 0)
    load_own = pltpu.make_async_copy(x_hbm, tok.at[z, y], tok_sem)
    load_own.start()
    for b in range(2):
        share_own(b)

    n_exp = n_rank * n_loc
    row = lax.broadcasted_iota(jnp.int32, (n_exp, tok_loc), 0)
    square = (tok_loc, tok_loc)
    before = jnp.where(lax.broadcasted_iota(jnp.int32, square, 0) < lax.broadcasted_iota(jnp.int32, square, 1), 1.0, 0.0).astype(BF16)

    def slot_map(expert_of_row):
        chosen = jnp.zeros((n_exp, tok_loc), F32)
        gates = jnp.zeros((n_exp, tok_loc), F32)
        for j in range(ids.shape[0]):
            hit = ids[j:j + 1, :] == expert_of_row
            chosen = jnp.where(hit, 1.0, chosen)
            gates = jnp.where(hit, gate_vals[j:j + 1, :], gates)
        slots = jnp.dot(chosen.astype(BF16), before, preferred_element_type=F32)
        return jnp.where((chosen > 0.5) & (slots < capacity - 0.5), slots, -1.0), gates

    slots_send[...] = slot_map(row)[0].reshape(slots_send.shape)
    slots, gates = slot_map(lax.rem(row, n_rank) * n_loc + row // n_rank)
    slots_own[...] = slots.reshape(slots_own.shape)
    gates_own[...] = gates.reshape(gates_own.shape)
    acc[...] = jnp.zeros_like(acc)
    for i in range(3):
        last_own(i).start()
    for s in range(2):
        for q in range(4):
            line_desc(q, s).wait_recv()
            line_start(q, s + 1)
        if s == 0:
            for j in range(1, n_rank):
                remote(slots_send.at[peer(j)], meta.at[ep], meta_s.at[j], meta_r.at[j], ep=peer(j)).start()
            meta[ep] = slots_send[ep]
    forward(0, 0)
    load_own.wait()
    for q in range(4):
        line_desc(q, 2).wait_recv()
    for q in range(4):
        plane_start(q, 0)
    forward(0, 1)
    send_first(2)
    forward(1, 0)
    for q in range(4):
        plane_desc(q, 0).wait_recv()
        plane_start(q, 1)
    forward(1, 1)
    forward(0, 2)
    send_first(3)
    for q in range(4):
        plane_desc(q, 1).wait_recv()
        plane_start(q, 2)
    for q in range(4):
        plane_desc(q, 2).wait_recv()
    for j in range(1, n_rank):
        remote(slots_send.at[back_peer(j)], meta.at[back_peer(j)], meta_s.at[j], meta_r.at[j], ep=peer(j)).wait_recv()

    @pl.loop(0, n_rank)
    def _(s):
        slot_iota = lax.broadcasted_iota(jnp.int32, (n_loc, capacity, tok_loc), 1).astype(F32)
        pick = jnp.where(meta[s][:, None, :] == slot_iota, 1.0, 0.0).reshape(n_loc * capacity, tok_loc).astype(BF16)
        picked = jnp.dot(pick, tok[s // RING, lax.rem(s, RING)], preferred_element_type=F32).astype(BF16)
        for e in range(n_loc):
            rows_in[e, src_rows(s), :] = picked[e * capacity:(e + 1) * capacity]

    forward(1, 2)

    @pl.loop(0, coarse - 2)
    def _(b):
        expert(b)

        @pl.when(b == 0)
        def _():
            forward(0, 3)
            send_first(4)

        @pl.when(b >= 2)
        def _():
            forward(1, b + 1)

        @pl.when(b >= 1)
        def _():
            combine(b - 1)

        @pl.when(b >= 2)
        def _():
            forward(0, b + 2)

        @pl.when(b == 2)
        def _():
            send_first(5)

        @pl.when(b == 3)
        def _():
            fine_first(parts6)

    expert(coarse - 2)
    forward(1, coarse - 1)
    combine(coarse - 3)
    fine_forward(0, parts6)
    fine_first(parts7[:1])
    fine_share_all(0, parts6)
    expert(coarse - 1)
    fine_forward(1, parts6)
    fine_first(parts7[1:] + down7)
    fine_share_all(1, parts6)
    combine(coarse - 2)

    fine_forward(2, parts6)
    loads = fine_load(0) + fine_load(1)
    for c in loads:
        c.wait()
    loads = fine_load(2)
    hidden_of(coarse, wbuf)
    fine_forward(0, parts7)
    fine_share_all(0, parts7)
    for j in range(1, n_rank):
        y_send(coarse - 2, 0, j).wait_send()
    for c in loads:
        c.wait()
    down_all(0, wbuf)
    y_own(coarse, 0).start()
    for j in range(1, n_rank):
        y_send(coarse, 0, j).start()

    fine_forward(1, parts7)
    fine_forward(0, down7)
    fine_share_all(1, parts7)
    fine_share_all(0, down7)
    combine(coarse - 1)
    for j in range(1, n_rank):
        y_send(coarse - 1, 1, j).wait_send()
    for i in range(3):
        last_own(i).wait()
    fine_forward(2, parts7)
    for q in parts7:
        fine_shared(q)
    last = coarse + 1
    hidden_third(last, wlast, 0)
    fine_forward(1, down7[:2])
    hidden_third(last, wlast, 1)
    fine_forward(1, down7[2:])
    fine_share_all(1, down7)
    hidden_third(last, wlast, 2)

    def last_block(n):
        fine_shared(down7[n])
        down(1, wlast, n)
        for j in range(1, n_rank):
            yb_send(n, j).start()
        blk = pl.ds(n * width, width)
        retlast[ep, :, blk] = ybuf[1, src_rows(ep), blk]

    fine_forward(2, down7[:1])
    for n in range(1, BLOCKS):
        fine_forward(2, down7[n:n + 1])
        last_block(n - 1)
    last_block(BLOCKS - 1)
    combine(coarse)
    parts = mix_parts(last)
    for j in range(1, n_rank):
        y_send(coarse, 0, j).wait_send()

    def out_copy(n):
        blk = pl.ds(n * width, width)
        return pltpu.make_async_copy(ybuf.at[0, pl.ds(0, tok_loc), blk], out.at[:, blk], out_sem.at[n])

    for n in range(BLOCKS):
        blk = pl.ds(n * width, width)
        for j in range(1, n_rank):
            yb_recv(n, j).wait_recv()
        ybuf[0, pl.ds(0, tok_loc), blk] = (acc[:, blk] + mixed(parts, retlast[:, :, blk])).astype(out.dtype)
        out_copy(n).start()

    for j in range(1, n_rank):
        for n in range(BLOCKS):
            yb_send(n, j).wait_send()
    for n in range(BLOCKS):
        out_copy(n).wait()
    for q in range(5 + BLOCKS):
        fine_share_own_desc(q).wait_send()
        for d in range(2):
            for s in range(3):
                fine_desc(d, s, q).wait_send()
                fine_share_desc(d, s, q).wait_send()
    for q in range(4):
        for s in range(3):
            line_desc(q, s).wait_send()
            plane_desc(q, s).wait_send()
    for j in range(1, n_rank):
        remote(slots_send.at[peer(j)], meta.at[ep], meta_s.at[j], meta_r.at[j], ep=peer(j)).wait_send()

    @pl.loop(0, coarse)
    def _(e):
        share_own_desc(e).wait_send()
        for d in range(2):
            for s in range(3):
                ring_desc(d, s, e).wait_send()
                share_desc(d, s, e).wait_send()


def solution(mesh):
    expert_ranks = mesh.shape["ep"]
    row_spec = P(("dp", "ep", "tp"), None)

    def local_layer(x_loc, ids_loc, gate_loc, wg_loc, wu_loc, wd_loc):
        tok_loc, d_model = x_loc.shape
        n_top = ids_loc.shape[1]
        local_exp, _, cols = wg_loc.shape
        ffn = cols * mesh.shape["tp"]
        n_exp = local_exp * expert_ranks
        capacity = CAP_FACTOR * n_top * tok_loc // n_exp
        n_rows = expert_ranks * capacity
        any_spec = pl.BlockSpec(memory_space=pl.ANY)
        vmem_spec = pl.BlockSpec(memory_space=pltpu.VMEM)
        dma = pltpu.SemaphoreType.DMA
        out = pl.pallas_call(
            functools.partial(moe_kernel, expert_ranks, local_exp, capacity),
            out_shape=(
                jax.ShapeDtypeStruct((tok_loc, d_model), BF16),
                jax.ShapeDtypeStruct((local_exp - 1, 3, ffn, d_model), BF16),
                jax.ShapeDtypeStruct((local_exp - 1, expert_ranks, capacity, d_model), BF16),
            ),
            in_specs=[any_spec] * 4 + [vmem_spec] * 2,
            out_specs=(any_spec, any_spec, any_spec),
            scratch_shapes=[
                pltpu.VMEM((RING, RING, tok_loc, d_model), BF16),
                pltpu.VMEM((expert_ranks, local_exp, tok_loc), F32),
                pltpu.VMEM((expert_ranks, local_exp, tok_loc), F32),
                pltpu.VMEM((local_exp, expert_ranks, tok_loc), F32),
                pltpu.VMEM((local_exp, expert_ranks, tok_loc), F32),
                pltpu.VMEM((local_exp, n_rows, d_model), BF16),
                pltpu.VMEM((3, ffn, d_model), BF16),
                pltpu.VMEM((3, ffn, d_model), BF16),
                pltpu.VMEM((2, n_rows, d_model), BF16),
                pltpu.VMEM((expert_ranks, capacity, d_model), BF16),
                pltpu.VMEM((expert_ranks, capacity, d_model), BF16),
                pltpu.VMEM((n_rows, ffn), BF16),
                pltpu.VMEM((tok_loc, d_model), F32),
                dma((2, 3, local_exp - 2)),
                dma((2, 3, local_exp - 2)),
                dma((7, local_exp - 2)),
                dma((7, local_exp - 2)),
                dma((2, 3, 5 + BLOCKS)),
                dma((2, 3, 5 + BLOCKS)),
                dma((7, 5 + BLOCKS)),
                dma((7, 5 + BLOCKS)),
                dma((4, 3)),
                dma((4, 3)),
                dma((4, 3)),
                dma((4, 3)),
                dma((expert_ranks,)),
                dma((expert_ranks,)),
                dma((2, expert_ranks)),
                dma((local_exp, expert_ranks)),
                dma((BLOCKS, expert_ranks)),
                dma((BLOCKS, expert_ranks)),
                dma((3, 8)),
                dma((3,)),
                dma((2,)),
                dma,
                dma((BLOCKS,)),
                dma,
            ],
            compiler_params=pltpu.CompilerParams(collective_id=0, has_side_effects=True, vmem_limit_bytes=67000000),
        )(
            x_loc,
            jnp.swapaxes(wg_loc, 1, 2),
            jnp.swapaxes(wu_loc, 1, 2),
            wd_loc,
            ids_loc.T,
            gate_loc.T,
        )
        return out[0]

    return jax.shard_map(local_layer, mesh=mesh, in_specs=(row_spec, row_spec, row_spec, P("ep", None, "tp"), P("ep", None, "tp"), P("ep", "tp", None)), out_specs=row_spec, check_vma=False)
```

```python
import functools

import jax
import jax.numpy as jnp
from jax import lax
from jax.experimental import pallas as pl
from jax.experimental.pallas import tpu as pltpu
from jax.sharding import PartitionSpec as P

CAP_FACTOR = 2
RING = 4
CORES = 2
MESH = pl.DeviceIdType.MESH
F32 = jnp.float32
BF16 = jnp.bfloat16


ROUND = ((0, 1), (0, -1), (1, 0), (-1, 0), (2, 2), (1, 1), (-1, -1), (1, -1), (-1, 1), (0, 2), (2, 0), (2, 1), (1, 2), (2, -1), (-1, 2))
BLOCKS = 4


def remote(src, dst, send, recv, **device):
    return pltpu.make_async_remote_copy(src_ref=src, dst_ref=dst, send_sem=send, recv_sem=recv, device_id=device, device_id_type=MESH)


def moe_kernel(n_rank, n_loc, capacity, x_hbm, wg, wu, wd, ids, gate_vals, out, wfull, yret, tok, meta, slots_send, slots_own, gates_own, rows_in, wbuf, wlast, ybuf, retbuf, retlast, hid, acc, ring_s, ring_r, part_s, part_r, fine_s, fine_r, fpart_s, fpart_r, line_s, line_r, plane_s, plane_r, meta_s, meta_r, y_s, y_r, yb_s, yb_r, load_sem, last_sem, own_sem, ret_sem, out_sem, tok_sem):
    ep = lax.axis_index("ep")
    tp = lax.axis_index("tp")
    z, y = ep // RING, lax.rem(ep, RING)
    x, core = tp // CORES, lax.rem(tp, CORES)
    weights = (wg, wu, wd)
    cols = wg.shape[1]
    half = cols // 2
    tok_loc = x_hbm.shape[0]
    quart = tok_loc // 4
    n_rows = n_rank * capacity

    def step(pos, amount):
        return lax.rem(pos + amount + 2 * RING, RING)

    ring_to = (step(x, 1) * CORES + core, step(x, -1) * CORES + core)
    partner = x * CORES + 1 - core

    def chunk_rows(t, d):
        return pl.ds(pl.multiple_of(t * cols + d * half, 16), half)

    def ring_in_x(d, s):
        return step(x, -1 - s) if d == 0 else step(x, 1 + s)

    def ring_start(d, s, e):
        if s == 0:
            rows = chunk_rows(tp, d)
            for i, w in enumerate(weights):
                remote(w.at[e, pl.ds(d * half, half), :], wfull.at[e, i, rows, :], ring_s.at[d, s, e], ring_r.at[d, s, e], tp=ring_to[d]).start()
        else:
            piece = wfull.at[e, :, chunk_rows(ring_in_x(d, s - 1) * CORES + core, d), :]
            remote(piece, piece, ring_s.at[d, s, e], ring_r.at[d, s, e], tp=ring_to[d]).start()

    def ring_desc(d, s, e):
        piece = wfull.at[e, :, chunk_rows(ring_in_x(d, s) * CORES + core, d), :]
        return remote(piece, piece, ring_s.at[d, s, e], ring_r.at[d, s, e], tp=ring_to[d])

    def own_rows(t):
        return pl.ds(pl.multiple_of(t * cols, 16), cols)

    def share_own(e):
        for i, w in enumerate(weights):
            remote(w.at[e], wfull.at[e, i, own_rows(tp), :], part_s.at[6, e], part_r.at[6, e], tp=partner).start()

    def share_own_desc(e):
        piece = wfull.at[e, :, own_rows(partner), :]
        return remote(piece, piece, part_s.at[6, e], part_r.at[6, e], tp=partner)

    def share(d, s, e):
        piece = wfull.at[e, :, chunk_rows(ring_in_x(d, s) * CORES + core, d), :]
        remote(piece, piece, part_s.at[d * 3 + s, e], part_r.at[d * 3 + s, e], tp=partner).start()

    def share_desc(d, s, e):
        piece = wfull.at[e, :, chunk_rows(ring_in_x(d, s) * CORES + 1 - core, d), :]
        return remote(piece, piece, part_s.at[d * 3 + s, e], part_r.at[d * 3 + s, e], tp=partner)

    coarse = n_loc - 2
    width = x_hbm.shape[1] // BLOCKS
    third = wbuf.shape[1] // 3
    parts6 = (0, 1, 2)
    parts7 = (3, 4)
    down7 = tuple(range(5, 5 + BLOCKS))

    def fine_at(q):
        if q < 3:
            return coarse, q, slice(None)
        if q < 5:
            return coarse + 1, q - 3, slice(None)
        return coarse + 1, 2, pl.ds((q - 5) * width, width)

    def fine_own(q, rows):
        e, i, c = fine_at(q)
        return weights[i].at[e, rows, c]

    def fine_land(q, rows):
        e, i, c = fine_at(q)
        return wfull.at[e, i, rows, c] if q < 3 else wlast.at[i, rows, c]

    def fine_start(d, s, q):
        if s == 0:
            src, dst = fine_own(q, pl.ds(d * half, half)), fine_land(q, chunk_rows(tp, d))
        else:
            src = dst = fine_land(q, chunk_rows(ring_in_x(d, s - 1) * CORES + core, d))
        remote(src, dst, fine_s.at[d, s, q], fine_r.at[d, s, q], tp=ring_to[d]).start()

    def fine_desc(d, s, q):
        piece = fine_land(q, chunk_rows(ring_in_x(d, s) * CORES + core, d))
        return remote(piece, piece, fine_s.at[d, s, q], fine_r.at[d, s, q], tp=ring_to[d])

    def fine_share_own(q):
        remote(fine_own(q, pl.ds(0, cols)), fine_land(q, own_rows(tp)), fpart_s.at[6, q], fpart_r.at[6, q], tp=partner).start()

    def fine_share_own_desc(q):
        piece = fine_land(q, own_rows(partner))
        return remote(piece, piece, fpart_s.at[6, q], fpart_r.at[6, q], tp=partner)

    def fine_share(d, s, q):
        piece = fine_land(q, chunk_rows(ring_in_x(d, s) * CORES + core, d))
        remote(piece, piece, fpart_s.at[d * 3 + s, q], fpart_r.at[d * 3 + s, q], tp=partner).start()

    def fine_share_desc(d, s, q):
        piece = fine_land(q, chunk_rows(ring_in_x(d, s) * CORES + 1 - core, d))
        return remote(piece, piece, fpart_s.at[d * 3 + s, q], fpart_r.at[d * 3 + s, q], tp=partner)

    def fine_forward(s, items):
        for q in items:
            for d in range(2):
                fine_desc(d, s, q).wait_recv()
                if s < 2:
                    fine_start(d, s + 1, q)
                else:
                    fine_share(d, s, q)

    def fine_share_all(s, items):
        for q in items:
            for d in range(2):
                fine_share(d, s, q)

    def fine_shared(q):
        fine_share_own_desc(q).wait_recv()
        for d in range(2):
            for s in range(3):
                fine_share_desc(d, s, q).wait_recv()

    def last_own(i):
        return pltpu.make_async_copy(weights[i].at[coarse + 1], wlast.at[i, own_rows(tp), :], last_sem.at[i])

    def fine_load(q):
        fine_shared(q)
        e, i, c = fine_at(q)
        copies = [pltpu.make_async_copy(fine_own(q, pl.ds(0, cols)), wbuf.at[i, own_rows(tp), c], load_sem.at[q, 0])]
        for j in range(1, RING * CORES):
            other = own_rows(lax.rem(tp + j, RING * CORES))
            copies.append(pltpu.make_async_copy(fine_land(q, other), wbuf.at[i, other, c], load_sem.at[q, j]))
        for c in copies:
            c.start()
        return copies

    routes = (("y", 1), ("y", -1), ("z", 1), ("z", -1))

    def plane_peer(axis, amount):
        return z * RING + step(y, amount) if axis == "y" else step(z, amount) * RING + y

    def quarter(q):
        return pl.ds(q * quart, quart)

    def line_piece(q, back):
        axis, sign = routes[q]
        if axis == "y":
            return tok.at[z, step(y, -sign * back), quarter(q), :]
        return tok.at[step(z, -sign * back), y, quarter(q), :]

    def line_start(q, s):
        axis, sign = routes[q]
        src = x_hbm.at[quarter(q), :] if s == 0 else line_piece(q, s)
        remote(src, line_piece(q, s), line_s.at[q, s], line_r.at[q, s], ep=plane_peer(axis, sign)).start()

    def line_desc(q, s):
        axis, sign = routes[q]
        piece = line_piece(q, s + 1)
        return remote(piece, piece, line_s.at[q, s], line_r.at[q, s], ep=plane_peer(axis, sign))

    def plane_piece(q, back):
        axis, sign = routes[q]
        if axis == "y":
            return tok.at[step(z, -sign * back), :, quarter(q), :]
        return tok.at[:, step(y, -sign * back), quarter(q), :]

    def plane_start(q, s):
        axis, sign = routes[q]
        piece = plane_piece(q, s)
        remote(piece, piece, plane_s.at[q, s], plane_r.at[q, s], ep=plane_peer("z" if axis == "y" else "y", sign)).start()

    def plane_desc(q, s):
        axis, sign = routes[q]
        piece = plane_piece(q, s + 1)
        return remote(piece, piece, plane_s.at[q, s], plane_r.at[q, s], ep=plane_peer("z" if axis == "y" else "y", sign))

    def peer(j):
        dz, dy = ROUND[j - 1]
        return step(z, dz) * RING + step(y, dy)

    def back_peer(j):
        dz, dy = ROUND[j - 1]
        return step(z, -dz) * RING + step(y, -dy)

    def src_rows(r):
        return pl.ds(pl.multiple_of(r * capacity, capacity), capacity)

    def y_send(e, k, j):
        r = peer(j)
        return remote(ybuf.at[k, src_rows(r), :], yret.at[e, ep], y_s.at[k, j], y_r.at[e, j], ep=r)

    def y_recv(e, j):
        r = back_peer(j)
        return remote(yret.at[e, r], yret.at[e, r], y_s.at[0, j], y_r.at[e, j], ep=peer(j))

    def y_own(e, k):
        return pltpu.make_async_copy(ybuf.at[k, src_rows(ep), :], yret.at[e, ep], own_sem.at[k])

    def yb_send(n, j):
        r, c = peer(j), pl.ds(n * width, width)
        return remote(ybuf.at[1, src_rows(r), c], retlast.at[ep, :, c], yb_s.at[n, j], yb_r.at[n, j], ep=r)

    def yb_recv(n, j):
        r, c = back_peer(j), pl.ds(n * width, width)
        piece = retlast.at[r, :, c]
        return remote(piece, piece, yb_s.at[n, j], yb_r.at[n, j], ep=peer(j))

    barrier = pltpu.get_barrier_semaphore()
    for j in range(1, n_rank):
        pl.semaphore_signal(barrier, inc=1, device_id={"ep": peer(j)}, device_id_type=MESH)
    for t in (*ring_to, partner):
        pl.semaphore_signal(barrier, inc=1, device_id={"tp": t}, device_id_type=MESH)
    pl.semaphore_wait(barrier, n_rank - 1 + 3)

    def ring_issue(b, static):
        def when(cond, fn):
            if static:
                if cond:
                    fn()
            else:
                pl.when(cond)(fn)

        def first():
            for d in range(2):
                ring_desc(d, 0, b).wait_recv()
                ring_start(d, 1, b)
            for d in range(2):
                share(d, 0, b)

        def second():
            for d in range(2):
                ring_desc(d, 1, b - 1).wait_recv()
                ring_start(d, 2, b - 1)
            for d in range(2):
                share(d, 1, b - 1)

        def ahead():
            for d in range(2):
                ring_start(d, 0, b + 2)
            share_own(b + 2)

        def ahead_fine():
            for q in parts6:
                for d in range(2):
                    fine_start(d, 0, q)
            for q in parts6:
                fine_share_own(q)

        first()
        if static:
            if 1 <= b:
                second()
        else:
            second()
        when(b + 2 < coarse, ahead)
        when(b + 2 == coarse, ahead_fine)

    def mix_parts(e):
        slot_iota = lax.broadcasted_iota(jnp.int32, (n_rank, capacity, tok_loc), 1).astype(F32)
        place = slots_own[e][:, None, :] == slot_iota
        mix = jnp.where(place, gates_own[e][:, None, :], 0.0).reshape(n_rows, tok_loc).T
        hi = mix.astype(BF16)
        rest = mix - hi.astype(F32)
        mid = rest.astype(BF16)
        low = (rest - mid.astype(F32)).astype(BF16)
        return hi, mid, low

    def mixed(parts, ret):
        ret = ret.reshape(n_rows, width)
        hi, mid, low = (jnp.dot(p, ret, preferred_element_type=F32) for p in parts)
        return hi + mid + low

    def combine(e):
        for j in range(1, n_rank):
            y_recv(e, j).wait_recv()
        y_own(e, e % 2 if isinstance(e, int) else lax.rem(e, 2)).wait()
        load = pltpu.make_async_copy(yret.at[e], retbuf, ret_sem)
        load.start()
        parts = mix_parts(e)
        load.wait()
        for n in range(BLOCKS):
            blk = pl.ds(n * width, width)
            acc[:, blk] += mixed(parts, retbuf[:, :, blk])

    def hidden_third(e, w, f):
        blk = pl.ds(pl.multiple_of(f * third, third) if not isinstance(f, int) else f * third, third)
        dims = (((1,), (1,)), ((), ()))
        xe = rows_in[e]
        a = lax.dot_general(xe, w[0, blk, :], dims, preferred_element_type=F32)
        b = lax.dot_general(xe, w[1, blk, :], dims, preferred_element_type=F32)
        hid[:, blk] = (jax.nn.silu(a) * b).astype(BF16)

    def hidden_of(e, w):
        @pl.loop(0, 3)
        def _(f):
            hidden_third(e, w, f)

    def down(k, w, n):
        blk = pl.ds(pl.multiple_of(n * width, width) if not isinstance(n, int) else n * width, width)
        ybuf[k, :, blk] = jnp.dot(hid[...], w[2, :, blk], preferred_element_type=F32).astype(BF16)

    def down_all(k, w):
        @pl.loop(0, BLOCKS)
        def _(n):
            down(k, w, n)

    def expert(e, before_hidden=None, before_down=None):
        for d in range(2):
            ring_desc(d, 2, e).wait_recv()
            share(d, 2, e)
        share_own_desc(e).wait_recv()
        for d in range(2):
            for s in range(3):
                share_desc(d, s, e).wait_recv()
        copies = []
        for i, w in enumerate(weights):
            copies.append(pltpu.make_async_copy(w.at[e], wbuf.at[i, own_rows(tp), :], load_sem.at[0, i]))
        for j in range(1, RING * CORES):
            other = own_rows(lax.rem(tp + j, RING * CORES))
            copies.append(pltpu.make_async_copy(wfull.at[e, :, other, :], wbuf.at[:, other, :], load_sem.at[1, j]))
        for c in copies:
            c.start()
        k = e % 2 if isinstance(e, int) else lax.rem(e, 2)

        def free_slot():
            for j in range(1, n_rank):
                y_send(e - 2, k, j).wait_send()

        if isinstance(e, int):
            free_slot()
        else:
            pl.when(e >= 2)(free_slot)

        for c in copies:
            c.wait()
        if before_hidden is not None:
            before_hidden()
        hidden_of(e, wbuf)
        if before_down is not None:
            before_down()
        down_all(k, wbuf)
        y_own(e, k).start()
        for j in range(1, n_rank):
            y_send(e, k, j).start()

    for b in range(2):
        for d in range(2):
            ring_start(d, 0, b)
    for q in range(4):
        line_start(q, 0)
    load_own = pltpu.make_async_copy(x_hbm, tok.at[z, y], tok_sem)
    load_own.start()
    for b in range(2):
        share_own(b)

    n_exp = n_rank * n_loc
    row = lax.broadcasted_iota(jnp.int32, (n_exp, tok_loc), 0)
    square = (tok_loc, tok_loc)
    before = jnp.where(lax.broadcasted_iota(jnp.int32, square, 0) < lax.broadcasted_iota(jnp.int32, square, 1), 1.0, 0.0).astype(BF16)

    def slot_map(expert_of_row):
        chosen = jnp.zeros((n_exp, tok_loc), F32)
        gates = jnp.zeros((n_exp, tok_loc), F32)
        for j in range(ids.shape[0]):
            hit = ids[j:j + 1, :] == expert_of_row
            chosen = jnp.where(hit, 1.0, chosen)
            gates = jnp.where(hit, gate_vals[j:j + 1, :], gates)
        slots = jnp.dot(chosen.astype(BF16), before, preferred_element_type=F32)
        return jnp.where((chosen > 0.5) & (slots < capacity - 0.5), slots, -1.0), gates

    slots_send[...] = slot_map(row)[0].reshape(slots_send.shape)
    slots, gates = slot_map(lax.rem(row, n_rank) * n_loc + row // n_rank)
    slots_own[...] = slots.reshape(slots_own.shape)
    gates_own[...] = gates.reshape(gates_own.shape)
    acc[...] = jnp.zeros_like(acc)
    for i in range(3):
        last_own(i).start()
    for s in range(2):
        for q in range(4):
            line_desc(q, s).wait_recv()
            line_start(q, s + 1)
        if s == 0:
            for j in range(1, n_rank):
                remote(slots_send.at[peer(j)], meta.at[ep], meta_s.at[j], meta_r.at[j], ep=peer(j)).start()
            meta[ep] = slots_send[ep]
    ring_issue(0, True)
    load_own.wait()
    for q in range(4):
        line_desc(q, 2).wait_recv()
    for q in range(4):
        plane_start(q, 0)
    ring_issue(1, True)
    for q in range(4):
        plane_desc(q, 0).wait_recv()
        plane_start(q, 1)
    ring_issue(2, True)
    for q in range(4):
        plane_desc(q, 1).wait_recv()
        plane_start(q, 2)
    for q in range(4):
        plane_desc(q, 2).wait_recv()
    for j in range(1, n_rank):
        remote(slots_send.at[back_peer(j)], meta.at[back_peer(j)], meta_s.at[j], meta_r.at[j], ep=peer(j)).wait_recv()

    @pl.loop(0, n_rank)
    def _(s):
        slot_iota = lax.broadcasted_iota(jnp.int32, (n_loc, capacity, tok_loc), 1).astype(F32)
        pick = jnp.where(meta[s][:, None, :] == slot_iota, 1.0, 0.0).reshape(n_loc * capacity, tok_loc).astype(BF16)
        picked = jnp.dot(pick, tok[s // RING, lax.rem(s, RING)], preferred_element_type=F32).astype(BF16)
        for e in range(n_loc):
            rows_in[e, src_rows(s), :] = picked[e * capacity:(e + 1) * capacity]

    @pl.loop(2, coarse)
    def _(b):
        @pl.when(b > 2)
        def _():
            ring_issue(b, False)

        expert(b - 2)

        @pl.when(b > 2)
        def _():
            combine(b - 3)

    for d in range(2):
        ring_desc(d, 1, coarse - 1).wait_recv()
        ring_start(d, 2, coarse - 1)
        share(d, 1, coarse - 1)
    fine_forward(0, parts6)
    fine_share_all(0, parts6)
    expert(coarse - 2)
    combine(coarse - 3)
    expert(coarse - 1, lambda: fine_forward(1, parts6[:1]), lambda: fine_forward(1, parts6[1:2]))
    fine_forward(1, parts6[2:])
    for q in parts7 + down7:
        for d in range(2):
            fine_start(d, 0, q)
    fine_share_all(1, parts6)
    for q in parts7 + down7:
        fine_share_own(q)
    combine(coarse - 2)

    fine_forward(2, parts6)
    loads = fine_load(0) + fine_load(1)
    for c in loads:
        c.wait()
    loads = fine_load(2)
    hidden_of(coarse, wbuf)
    fine_forward(0, parts7)
    fine_share_all(0, parts7)
    for j in range(1, n_rank):
        y_send(coarse - 2, 0, j).wait_send()
    for c in loads:
        c.wait()
    down_all(0, wbuf)
    y_own(coarse, 0).start()
    for j in range(1, n_rank):
        y_send(coarse, 0, j).start()

    fine_forward(1, parts7)
    fine_forward(0, down7)
    fine_share_all(1, parts7)
    fine_share_all(0, down7)
    combine(coarse - 1)
    for j in range(1, n_rank):
        y_send(coarse - 1, 1, j).wait_send()
    for i in range(3):
        last_own(i).wait()
    fine_forward(2, parts7)
    for q in parts7:
        fine_shared(q)
    last = coarse + 1
    hidden_third(last, wlast, 0)
    fine_forward(1, down7[:2])
    hidden_third(last, wlast, 1)
    fine_forward(1, down7[2:])
    fine_share_all(1, down7)
    hidden_third(last, wlast, 2)

    def last_block(n):
        fine_shared(down7[n])
        down(1, wlast, n)
        for j in range(1, n_rank):
            yb_send(n, j).start()
        blk = pl.ds(n * width, width)
        retlast[ep, :, blk] = ybuf[1, src_rows(ep), blk]

    fine_forward(2, down7[:1])
    for n in range(1, BLOCKS):
        fine_forward(2, down7[n:n + 1])
        last_block(n - 1)
    last_block(BLOCKS - 1)
    combine(coarse)
    parts = mix_parts(last)
    for j in range(1, n_rank):
        y_send(coarse, 0, j).wait_send()

    def out_copy(n):
        blk = pl.ds(n * width, width)
        return pltpu.make_async_copy(ybuf.at[0, pl.ds(0, tok_loc), blk], out.at[:, blk], out_sem.at[n])

    for n in range(BLOCKS):
        blk = pl.ds(n * width, width)
        for j in range(1, n_rank):
            yb_recv(n, j).wait_recv()
        ybuf[0, pl.ds(0, tok_loc), blk] = (acc[:, blk] + mixed(parts, retlast[:, :, blk])).astype(out.dtype)
        out_copy(n).start()

    for j in range(1, n_rank):
        for n in range(BLOCKS):
            yb_send(n, j).wait_send()
    for n in range(BLOCKS):
        out_copy(n).wait()
    for q in range(5 + BLOCKS):
        fine_share_own_desc(q).wait_send()
        for d in range(2):
            for s in range(3):
                fine_desc(d, s, q).wait_send()
                fine_share_desc(d, s, q).wait_send()
    for q in range(4):
        for s in range(3):
            line_desc(q, s).wait_send()
            plane_desc(q, s).wait_send()
    for j in range(1, n_rank):
        remote(slots_send.at[peer(j)], meta.at[ep], meta_s.at[j], meta_r.at[j], ep=peer(j)).wait_send()

    @pl.loop(0, coarse)
    def _(e):
        share_own_desc(e).wait_send()
        for d in range(2):
            for s in range(3):
                ring_desc(d, s, e).wait_send()
                share_desc(d, s, e).wait_send()


def solution(mesh):
    expert_ranks = mesh.shape["ep"]
    row_spec = P(("dp", "ep", "tp"), None)

    def local_layer(x_loc, ids_loc, gate_loc, wg_loc, wu_loc, wd_loc):
        tok_loc, d_model = x_loc.shape
        n_top = ids_loc.shape[1]
        local_exp, _, cols = wg_loc.shape
        ffn = cols * mesh.shape["tp"]
        n_exp = local_exp * expert_ranks
        capacity = CAP_FACTOR * n_top * tok_loc // n_exp
        n_rows = expert_ranks * capacity
        any_spec = pl.BlockSpec(memory_space=pl.ANY)
        vmem_spec = pl.BlockSpec(memory_space=pltpu.VMEM)
        dma = pltpu.SemaphoreType.DMA
        out = pl.pallas_call(
            functools.partial(moe_kernel, expert_ranks, local_exp, capacity),
            out_shape=(
                jax.ShapeDtypeStruct((tok_loc, d_model), BF16),
                jax.ShapeDtypeStruct((local_exp - 1, 3, ffn, d_model), BF16),
                jax.ShapeDtypeStruct((local_exp - 1, expert_ranks, capacity, d_model), BF16),
            ),
            in_specs=[any_spec] * 4 + [vmem_spec] * 2,
            out_specs=(any_spec, any_spec, any_spec),
            scratch_shapes=[
                pltpu.VMEM((RING, RING, tok_loc, d_model), BF16),
                pltpu.VMEM((expert_ranks, local_exp, tok_loc), F32),
                pltpu.VMEM((expert_ranks, local_exp, tok_loc), F32),
                pltpu.VMEM((local_exp, expert_ranks, tok_loc), F32),
                pltpu.VMEM((local_exp, expert_ranks, tok_loc), F32),
                pltpu.VMEM((local_exp, n_rows, d_model), BF16),
                pltpu.VMEM((3, ffn, d_model), BF16),
                pltpu.VMEM((3, ffn, d_model), BF16),
                pltpu.VMEM((2, n_rows, d_model), BF16),
                pltpu.VMEM((expert_ranks, capacity, d_model), BF16),
                pltpu.VMEM((expert_ranks, capacity, d_model), BF16),
                pltpu.VMEM((n_rows, ffn), BF16),
                pltpu.VMEM((tok_loc, d_model), F32),
                dma((2, 3, local_exp - 2)),
                dma((2, 3, local_exp - 2)),
                dma((7, local_exp - 2)),
                dma((7, local_exp - 2)),
                dma((2, 3, 5 + BLOCKS)),
                dma((2, 3, 5 + BLOCKS)),
                dma((7, 5 + BLOCKS)),
                dma((7, 5 + BLOCKS)),
                dma((4, 3)),
                dma((4, 3)),
                dma((4, 3)),
                dma((4, 3)),
                dma((expert_ranks,)),
                dma((expert_ranks,)),
                dma((2, expert_ranks)),
                dma((local_exp, expert_ranks)),
                dma((BLOCKS, expert_ranks)),
                dma((BLOCKS, expert_ranks)),
                dma((3, 8)),
                dma((3,)),
                dma((2,)),
                dma,
                dma((BLOCKS,)),
                dma,
            ],
            compiler_params=pltpu.CompilerParams(collective_id=0, has_side_effects=True, vmem_limit_bytes=67000000),
        )(
            x_loc,
            jnp.swapaxes(wg_loc, 1, 2),
            jnp.swapaxes(wu_loc, 1, 2),
            wd_loc,
            ids_loc.T,
            gate_loc.T,
        )
        return out[0]

    return jax.shard_map(local_layer, mesh=mesh, in_specs=(row_spec, row_spec, row_spec, P("ep", None, "tp"), P("ep", None, "tp"), P("ep", "tp", None)), out_specs=row_spec, check_vma=False)
```

```python
import functools

import jax
import jax.numpy as jnp
from jax import lax
from jax.experimental import pallas as pl
from jax.experimental.pallas import tpu as pltpu
from jax.sharding import PartitionSpec as P

CAP_FACTOR = 2
RING = 4
CORES = 2
MESH = pl.DeviceIdType.MESH
F32 = jnp.float32
BF16 = jnp.bfloat16


ROUND = ((0, 1), (0, -1), (1, 0), (-1, 0), (2, 2), (1, 1), (-1, -1), (1, -1), (-1, 1), (0, 2), (2, 0), (2, 1), (1, 2), (2, -1), (-1, 2))
BLOCKS = 4


def remote(src, dst, send, recv, **device):
    return pltpu.make_async_remote_copy(src_ref=src, dst_ref=dst, send_sem=send, recv_sem=recv, device_id=device, device_id_type=MESH)


def moe_kernel(n_rank, n_loc, capacity, x_hbm, wg, wu, wd, ids, gate_vals, out, wfull, yret, tok, meta, slots_send, slots_own, gates_own, rows_in, wbuf, wlast, ybuf, retbuf, retlast, hid, acc, ring_s, ring_r, part_s, part_r, fine_s, fine_r, fpart_s, fpart_r, line_s, line_r, plane_s, plane_r, meta_s, meta_r, y_s, y_r, yb_s, yb_r, load_sem, last_sem, own_sem, ret_sem, out_sem, tok_sem):
    ep = lax.axis_index("ep")
    tp = lax.axis_index("tp")
    z, y = ep // RING, lax.rem(ep, RING)
    x, core = tp // CORES, lax.rem(tp, CORES)
    weights = (wg, wu, wd)
    cols = wg.shape[1]
    half = cols // 2
    tok_loc = x_hbm.shape[0]
    quart = tok_loc // 4
    n_rows = n_rank * capacity

    def step(pos, amount):
        return lax.rem(pos + amount + 2 * RING, RING)

    ring_to = (step(x, 1) * CORES + core, step(x, -1) * CORES + core)
    partner = x * CORES + 1 - core

    def chunk_rows(t, d):
        return pl.ds(pl.multiple_of(t * cols + d * half, 16), half)

    def ring_in_x(d, s):
        return step(x, -1 - s) if d == 0 else step(x, 1 + s)

    def ring_start(d, s, e):
        if s == 0:
            rows = chunk_rows(tp, d)
            for i, w in enumerate(weights):
                remote(w.at[e, pl.ds(d * half, half), :], wfull.at[e, i, rows, :], ring_s.at[d, s, e], ring_r.at[d, s, e], tp=ring_to[d]).start()
        else:
            piece = wfull.at[e, :, chunk_rows(ring_in_x(d, s - 1) * CORES + core, d), :]
            remote(piece, piece, ring_s.at[d, s, e], ring_r.at[d, s, e], tp=ring_to[d]).start()

    def ring_desc(d, s, e):
        piece = wfull.at[e, :, chunk_rows(ring_in_x(d, s) * CORES + core, d), :]
        return remote(piece, piece, ring_s.at[d, s, e], ring_r.at[d, s, e], tp=ring_to[d])

    def own_rows(t):
        return pl.ds(pl.multiple_of(t * cols, 16), cols)

    def share_own(e):
        for i, w in enumerate(weights):
            remote(w.at[e], wfull.at[e, i, own_rows(tp), :], part_s.at[6, e], part_r.at[6, e], tp=partner).start()

    def share_own_desc(e):
        piece = wfull.at[e, :, own_rows(partner), :]
        return remote(piece, piece, part_s.at[6, e], part_r.at[6, e], tp=partner)

    def share(d, s, e):
        piece = wfull.at[e, :, chunk_rows(ring_in_x(d, s) * CORES + core, d), :]
        remote(piece, piece, part_s.at[d * 3 + s, e], part_r.at[d * 3 + s, e], tp=partner).start()

    def share_desc(d, s, e):
        piece = wfull.at[e, :, chunk_rows(ring_in_x(d, s) * CORES + 1 - core, d), :]
        return remote(piece, piece, part_s.at[d * 3 + s, e], part_r.at[d * 3 + s, e], tp=partner)

    coarse = n_loc - 2
    width = x_hbm.shape[1] // BLOCKS
    third = wbuf.shape[1] // 3
    parts6 = (0, 1, 2)
    parts7 = (3, 4)
    down7 = tuple(range(5, 5 + BLOCKS))

    def fine_at(q):
        if q < 3:
            return coarse, q, slice(None)
        if q < 5:
            return coarse + 1, q - 3, slice(None)
        return coarse + 1, 2, pl.ds((q - 5) * width, width)

    def fine_own(q, rows):
        e, i, c = fine_at(q)
        return weights[i].at[e, rows, c]

    def fine_land(q, rows):
        e, i, c = fine_at(q)
        return wfull.at[e, i, rows, c] if q < 3 else wlast.at[i, rows, c]

    def fine_start(d, s, q):
        if s == 0:
            src, dst = fine_own(q, pl.ds(d * half, half)), fine_land(q, chunk_rows(tp, d))
        else:
            src = dst = fine_land(q, chunk_rows(ring_in_x(d, s - 1) * CORES + core, d))
        remote(src, dst, fine_s.at[d, s, q], fine_r.at[d, s, q], tp=ring_to[d]).start()

    def fine_desc(d, s, q):
        piece = fine_land(q, chunk_rows(ring_in_x(d, s) * CORES + core, d))
        return remote(piece, piece, fine_s.at[d, s, q], fine_r.at[d, s, q], tp=ring_to[d])

    def fine_share_own(q):
        remote(fine_own(q, pl.ds(0, cols)), fine_land(q, own_rows(tp)), fpart_s.at[6, q], fpart_r.at[6, q], tp=partner).start()

    def fine_share_own_desc(q):
        piece = fine_land(q, own_rows(partner))
        return remote(piece, piece, fpart_s.at[6, q], fpart_r.at[6, q], tp=partner)

    def fine_share(d, s, q):
        piece = fine_land(q, chunk_rows(ring_in_x(d, s) * CORES + core, d))
        remote(piece, piece, fpart_s.at[d * 3 + s, q], fpart_r.at[d * 3 + s, q], tp=partner).start()

    def fine_share_desc(d, s, q):
        piece = fine_land(q, chunk_rows(ring_in_x(d, s) * CORES + 1 - core, d))
        return remote(piece, piece, fpart_s.at[d * 3 + s, q], fpart_r.at[d * 3 + s, q], tp=partner)

    def fine_forward(s, items):
        for q in items:
            for d in range(2):
                fine_desc(d, s, q).wait_recv()
                if s < 2:
                    fine_start(d, s + 1, q)
                else:
                    fine_share(d, s, q)

    def fine_share_all(s, items):
        for q in items:
            for d in range(2):
                fine_share(d, s, q)

    def fine_shared(q):
        fine_share_own_desc(q).wait_recv()
        for d in range(2):
            for s in range(3):
                fine_share_desc(d, s, q).wait_recv()

    def last_own(i):
        return pltpu.make_async_copy(weights[i].at[coarse + 1], wlast.at[i, own_rows(tp), :], last_sem.at[i])

    def fine_load(q):
        fine_shared(q)
        e, i, c = fine_at(q)
        copies = [pltpu.make_async_copy(fine_own(q, pl.ds(0, cols)), wbuf.at[i, own_rows(tp), c], load_sem.at[q, 0])]
        for j in range(1, RING * CORES):
            other = own_rows(lax.rem(tp + j, RING * CORES))
            copies.append(pltpu.make_async_copy(fine_land(q, other), wbuf.at[i, other, c], load_sem.at[q, j]))
        for c in copies:
            c.start()
        return copies

    routes = (("y", 1), ("y", -1), ("z", 1), ("z", -1))

    def plane_peer(axis, amount):
        return z * RING + step(y, amount) if axis == "y" else step(z, amount) * RING + y

    def quarter(q):
        return pl.ds(q * quart, quart)

    def line_piece(q, back):
        axis, sign = routes[q]
        if axis == "y":
            return tok.at[z, step(y, -sign * back), quarter(q), :]
        return tok.at[step(z, -sign * back), y, quarter(q), :]

    def line_start(q, s):
        axis, sign = routes[q]
        src = x_hbm.at[quarter(q), :] if s == 0 else line_piece(q, s)
        remote(src, line_piece(q, s), line_s.at[q, s], line_r.at[q, s], ep=plane_peer(axis, sign)).start()

    def line_desc(q, s):
        axis, sign = routes[q]
        piece = line_piece(q, s + 1)
        return remote(piece, piece, line_s.at[q, s], line_r.at[q, s], ep=plane_peer(axis, sign))

    def plane_piece(q, back):
        axis, sign = routes[q]
        if axis == "y":
            return tok.at[step(z, -sign * back), :, quarter(q), :]
        return tok.at[:, step(y, -sign * back), quarter(q), :]

    def plane_start(q, s):
        axis, sign = routes[q]
        piece = plane_piece(q, s)
        remote(piece, piece, plane_s.at[q, s], plane_r.at[q, s], ep=plane_peer("z" if axis == "y" else "y", sign)).start()

    def plane_desc(q, s):
        axis, sign = routes[q]
        piece = plane_piece(q, s + 1)
        return remote(piece, piece, plane_s.at[q, s], plane_r.at[q, s], ep=plane_peer("z" if axis == "y" else "y", sign))

    def peer(j):
        dz, dy = ROUND[j - 1]
        return step(z, dz) * RING + step(y, dy)

    def back_peer(j):
        dz, dy = ROUND[j - 1]
        return step(z, -dz) * RING + step(y, -dy)

    def src_rows(r):
        return pl.ds(pl.multiple_of(r * capacity, capacity), capacity)

    def y_send(e, k, j):
        r = peer(j)
        return remote(ybuf.at[k, src_rows(r), :], yret.at[e, ep], y_s.at[k, j], y_r.at[e, j], ep=r)

    def y_recv(e, j):
        r = back_peer(j)
        return remote(yret.at[e, r], yret.at[e, r], y_s.at[0, j], y_r.at[e, j], ep=peer(j))

    def y_own(e, k):
        return pltpu.make_async_copy(ybuf.at[k, src_rows(ep), :], yret.at[e, ep], own_sem.at[k])

    def yb_send(n, j):
        r, c = peer(j), pl.ds(n * width, width)
        return remote(ybuf.at[1, src_rows(r), c], retlast.at[ep, :, c], yb_s.at[n, j], yb_r.at[n, j], ep=r)

    def yb_recv(n, j):
        r, c = back_peer(j), pl.ds(n * width, width)
        piece = retlast.at[r, :, c]
        return remote(piece, piece, yb_s.at[n, j], yb_r.at[n, j], ep=peer(j))

    barrier = pltpu.get_barrier_semaphore()
    for j in range(1, n_rank):
        pl.semaphore_signal(barrier, inc=1, device_id={"ep": peer(j)}, device_id_type=MESH)
    for t in (*ring_to, partner):
        pl.semaphore_signal(barrier, inc=1, device_id={"tp": t}, device_id_type=MESH)
    pl.semaphore_wait(barrier, n_rank - 1 + 3)

    def send_first(e):
        for d in range(2):
            ring_start(d, 0, e)
        share_own(e)

    def forward(s, e):
        for d in range(2):
            ring_desc(d, s, e).wait_recv()
            ring_start(d, s + 1, e)
        for d in range(2):
            share(d, s, e)

    def fine_first(items):
        for q in items:
            for d in range(2):
                fine_start(d, 0, q)
        for q in items:
            fine_share_own(q)

    def mix_parts(e):
        slot_iota = lax.broadcasted_iota(jnp.int32, (n_rank, capacity, tok_loc), 1).astype(F32)
        place = slots_own[e][:, None, :] == slot_iota
        mix = jnp.where(place, gates_own[e][:, None, :], 0.0).reshape(n_rows, tok_loc).T
        hi = mix.astype(BF16)
        rest = mix - hi.astype(F32)
        mid = rest.astype(BF16)
        low = (rest - mid.astype(F32)).astype(BF16)
        return hi, mid, low

    def mixed(parts, ret):
        ret = ret.reshape(n_rows, width)
        hi, mid, low = (jnp.dot(p, ret, preferred_element_type=F32) for p in parts)
        return hi + mid + low

    def combine(e):
        for j in range(1, n_rank):
            y_recv(e, j).wait_recv()
        y_own(e, e % 2 if isinstance(e, int) else lax.rem(e, 2)).wait()
        load = pltpu.make_async_copy(yret.at[e], retbuf, ret_sem)
        load.start()
        parts = mix_parts(e)
        load.wait()
        for n in range(BLOCKS):
            blk = pl.ds(n * width, width)
            acc[:, blk] += mixed(parts, retbuf[:, :, blk])

    def hidden_third(e, w, f):
        blk = pl.ds(pl.multiple_of(f * third, third) if not isinstance(f, int) else f * third, third)
        dims = (((1,), (1,)), ((), ()))
        xe = rows_in[e]
        a = lax.dot_general(xe, w[0, blk, :], dims, preferred_element_type=F32)
        b = lax.dot_general(xe, w[1, blk, :], dims, preferred_element_type=F32)
        hid[:, blk] = (jax.nn.silu(a) * b).astype(BF16)

    def hidden_of(e, w):
        @pl.loop(0, 3)
        def _(f):
            hidden_third(e, w, f)

    def down(k, w, n):
        blk = pl.ds(pl.multiple_of(n * width, width) if not isinstance(n, int) else n * width, width)
        ybuf[k, :, blk] = jnp.dot(hid[...], w[2, :, blk], preferred_element_type=F32).astype(BF16)

    def down_all(k, w):
        @pl.loop(0, BLOCKS)
        def _(n):
            down(k, w, n)

    def expert(e, before_hidden=None, before_down=None):
        for d in range(2):
            ring_desc(d, 2, e).wait_recv()
            share(d, 2, e)
        share_own_desc(e).wait_recv()
        for d in range(2):
            for s in range(3):
                share_desc(d, s, e).wait_recv()
        copies = []
        for i, w in enumerate(weights):
            copies.append(pltpu.make_async_copy(w.at[e], wbuf.at[i, own_rows(tp), :], load_sem.at[0, i]))
        for j in range(1, RING * CORES):
            other = own_rows(lax.rem(tp + j, RING * CORES))
            copies.append(pltpu.make_async_copy(wfull.at[e, :, other, :], wbuf.at[:, other, :], load_sem.at[1, j]))
        for c in copies:
            c.start()
        k = e % 2 if isinstance(e, int) else lax.rem(e, 2)

        def free_slot():
            for j in range(1, n_rank):
                y_send(e - 2, k, j).wait_send()

        if isinstance(e, int):
            free_slot()
        else:
            pl.when(e >= 2)(free_slot)

        for c in copies:
            c.wait()
        if before_hidden is not None:
            before_hidden()
        hidden_of(e, wbuf)
        if before_down is not None:
            before_down()
        down_all(k, wbuf)
        y_own(e, k).start()
        for j in range(1, n_rank):
            y_send(e, k, j).start()

    for b in range(2):
        for d in range(2):
            ring_start(d, 0, b)
    for q in range(4):
        line_start(q, 0)
    load_own = pltpu.make_async_copy(x_hbm, tok.at[z, y], tok_sem)
    load_own.start()
    for b in range(2):
        share_own(b)

    n_exp = n_rank * n_loc
    row = lax.broadcasted_iota(jnp.int32, (n_exp, tok_loc), 0)
    square = (tok_loc, tok_loc)
    before = jnp.where(lax.broadcasted_iota(jnp.int32, square, 0) < lax.broadcasted_iota(jnp.int32, square, 1), 1.0, 0.0).astype(BF16)

    def slot_map(expert_of_row):
        chosen = jnp.zeros((n_exp, tok_loc), F32)
        gates = jnp.zeros((n_exp, tok_loc), F32)
        for j in range(ids.shape[0]):
            hit = ids[j:j + 1, :] == expert_of_row
            chosen = jnp.where(hit, 1.0, chosen)
            gates = jnp.where(hit, gate_vals[j:j + 1, :], gates)
        slots = jnp.dot(chosen.astype(BF16), before, preferred_element_type=F32)
        return jnp.where((chosen > 0.5) & (slots < capacity - 0.5), slots, -1.0), gates

    slots_send[...] = slot_map(row)[0].reshape(slots_send.shape)
    slots, gates = slot_map(lax.rem(row, n_rank) * n_loc + row // n_rank)
    slots_own[...] = slots.reshape(slots_own.shape)
    gates_own[...] = gates.reshape(gates_own.shape)
    acc[...] = jnp.zeros_like(acc)
    for i in range(3):
        last_own(i).start()
    for s in range(2):
        for q in range(4):
            line_desc(q, s).wait_recv()
            line_start(q, s + 1)
        if s == 0:
            for j in range(1, n_rank):
                remote(slots_send.at[peer(j)], meta.at[ep], meta_s.at[j], meta_r.at[j], ep=peer(j)).start()
            meta[ep] = slots_send[ep]
    forward(0, 0)
    load_own.wait()
    for q in range(4):
        line_desc(q, 2).wait_recv()
    for q in range(4):
        plane_start(q, 0)
    forward(0, 1)
    send_first(2)
    forward(1, 0)
    for q in range(4):
        plane_desc(q, 0).wait_recv()
        plane_start(q, 1)
    forward(1, 1)
    forward(0, 2)
    send_first(3)
    for q in range(4):
        plane_desc(q, 1).wait_recv()
        plane_start(q, 2)
    for q in range(4):
        plane_desc(q, 2).wait_recv()
    for j in range(1, n_rank):
        remote(slots_send.at[back_peer(j)], meta.at[back_peer(j)], meta_s.at[j], meta_r.at[j], ep=peer(j)).wait_recv()

    @pl.loop(0, n_rank)
    def _(s):
        slot_iota = lax.broadcasted_iota(jnp.int32, (n_loc, capacity, tok_loc), 1).astype(F32)
        pick = jnp.where(meta[s][:, None, :] == slot_iota, 1.0, 0.0).reshape(n_loc * capacity, tok_loc).astype(BF16)
        picked = jnp.dot(pick, tok[s // RING, lax.rem(s, RING)], preferred_element_type=F32).astype(BF16)
        for e in range(n_loc):
            rows_in[e, src_rows(s), :] = picked[e * capacity:(e + 1) * capacity]

    forward(1, 2)

    @pl.loop(0, coarse - 2)
    def _(b):
        expert(b)

        @pl.when(b == 0)
        def _():
            forward(0, 3)
            send_first(4)

        @pl.when(b >= 2)
        def _():
            forward(1, b + 1)

        @pl.when(b >= 1)
        def _():
            combine(b - 1)

        @pl.when(b >= 2)
        def _():
            forward(0, b + 2)

        @pl.when(b == 2)
        def _():
            send_first(5)

        @pl.when(b == 3)
        def _():
            fine_first(parts6)

    expert(coarse - 2)
    forward(1, coarse - 1)
    combine(coarse - 3)
    fine_forward(0, parts6)
    fine_share_all(0, parts6)
    expert(coarse - 1, lambda: fine_forward(1, parts6[:1]), lambda: fine_forward(1, parts6[1:2]))
    fine_forward(1, parts6[2:])
    fine_first(parts7 + down7)
    fine_share_all(1, parts6)
    combine(coarse - 2)

    fine_forward(2, parts6)
    loads = fine_load(0) + fine_load(1)
    for c in loads:
        c.wait()
    loads = fine_load(2)
    hidden_of(coarse, wbuf)
    fine_forward(0, parts7)
    fine_share_all(0, parts7)
    for j in range(1, n_rank):
        y_send(coarse - 2, 0, j).wait_send()
    for c in loads:
        c.wait()
    down_all(0, wbuf)
    y_own(coarse, 0).start()
    for j in range(1, n_rank):
        y_send(coarse, 0, j).start()

    fine_forward(1, parts7)
    fine_forward(0, down7)
    fine_share_all(1, parts7)
    fine_share_all(0, down7)
    combine(coarse - 1)
    for j in range(1, n_rank):
        y_send(coarse - 1, 1, j).wait_send()
    for i in range(3):
        last_own(i).wait()
    fine_forward(2, parts7)
    for q in parts7:
        fine_shared(q)
    last = coarse + 1
    hidden_third(last, wlast, 0)
    fine_forward(1, down7[:2])
    hidden_third(last, wlast, 1)
    fine_forward(1, down7[2:])
    fine_share_all(1, down7)
    hidden_third(last, wlast, 2)

    def last_block(n):
        fine_shared(down7[n])
        down(1, wlast, n)
        for j in range(1, n_rank):
            yb_send(n, j).start()
        blk = pl.ds(n * width, width)
        retlast[ep, :, blk] = ybuf[1, src_rows(ep), blk]

    fine_forward(2, down7[:1])
    for n in range(1, BLOCKS):
        fine_forward(2, down7[n:n + 1])
        last_block(n - 1)
    last_block(BLOCKS - 1)
    combine(coarse)
    parts = mix_parts(last)
    for j in range(1, n_rank):
        y_send(coarse, 0, j).wait_send()

    def out_copy(n):
        blk = pl.ds(n * width, width)
        return pltpu.make_async_copy(ybuf.at[0, pl.ds(0, tok_loc), blk], out.at[:, blk], out_sem.at[n])

    for n in range(BLOCKS):
        blk = pl.ds(n * width, width)
        for j in range(1, n_rank):
            yb_recv(n, j).wait_recv()
        ybuf[0, pl.ds(0, tok_loc), blk] = (acc[:, blk] + mixed(parts, retlast[:, :, blk])).astype(out.dtype)
        out_copy(n).start()

    for j in range(1, n_rank):
        for n in range(BLOCKS):
            yb_send(n, j).wait_send()
    for n in range(BLOCKS):
        out_copy(n).wait()
    for q in range(5 + BLOCKS):
        fine_share_own_desc(q).wait_send()
        for d in range(2):
            for s in range(3):
                fine_desc(d, s, q).wait_send()
                fine_share_desc(d, s, q).wait_send()
    for q in range(4):
        for s in range(3):
            line_desc(q, s).wait_send()
            plane_desc(q, s).wait_send()
    for j in range(1, n_rank):
        remote(slots_send.at[peer(j)], meta.at[ep], meta_s.at[j], meta_r.at[j], ep=peer(j)).wait_send()

    @pl.loop(0, coarse)
    def _(e):
        share_own_desc(e).wait_send()
        for d in range(2):
            for s in range(3):
                ring_desc(d, s, e).wait_send()
                share_desc(d, s, e).wait_send()


def solution(mesh):
    expert_ranks = mesh.shape["ep"]
    row_spec = P(("dp", "ep", "tp"), None)

    def local_layer(x_loc, ids_loc, gate_loc, wg_loc, wu_loc, wd_loc):
        tok_loc, d_model = x_loc.shape
        n_top = ids_loc.shape[1]
        local_exp, _, cols = wg_loc.shape
        ffn = cols * mesh.shape["tp"]
        n_exp = local_exp * expert_ranks
        capacity = CAP_FACTOR * n_top * tok_loc // n_exp
        n_rows = expert_ranks * capacity
        any_spec = pl.BlockSpec(memory_space=pl.ANY)
        vmem_spec = pl.BlockSpec(memory_space=pltpu.VMEM)
        dma = pltpu.SemaphoreType.DMA
        out = pl.pallas_call(
            functools.partial(moe_kernel, expert_ranks, local_exp, capacity),
            out_shape=(
                jax.ShapeDtypeStruct((tok_loc, d_model), BF16),
                jax.ShapeDtypeStruct((local_exp - 1, 3, ffn, d_model), BF16),
                jax.ShapeDtypeStruct((local_exp - 1, expert_ranks, capacity, d_model), BF16),
            ),
            in_specs=[any_spec] * 4 + [vmem_spec] * 2,
            out_specs=(any_spec, any_spec, any_spec),
            scratch_shapes=[
                pltpu.VMEM((RING, RING, tok_loc, d_model), BF16),
                pltpu.VMEM((expert_ranks, local_exp, tok_loc), F32),
                pltpu.VMEM((expert_ranks, local_exp, tok_loc), F32),
                pltpu.VMEM((local_exp, expert_ranks, tok_loc), F32),
                pltpu.VMEM((local_exp, expert_ranks, tok_loc), F32),
                pltpu.VMEM((local_exp, n_rows, d_model), BF16),
                pltpu.VMEM((3, ffn, d_model), BF16),
                pltpu.VMEM((3, ffn, d_model), BF16),
                pltpu.VMEM((2, n_rows, d_model), BF16),
                pltpu.VMEM((expert_ranks, capacity, d_model), BF16),
                pltpu.VMEM((expert_ranks, capacity, d_model), BF16),
                pltpu.VMEM((n_rows, ffn), BF16),
                pltpu.VMEM((tok_loc, d_model), F32),
                dma((2, 3, local_exp - 2)),
                dma((2, 3, local_exp - 2)),
                dma((7, local_exp - 2)),
                dma((7, local_exp - 2)),
                dma((2, 3, 5 + BLOCKS)),
                dma((2, 3, 5 + BLOCKS)),
                dma((7, 5 + BLOCKS)),
                dma((7, 5 + BLOCKS)),
                dma((4, 3)),
                dma((4, 3)),
                dma((4, 3)),
                dma((4, 3)),
                dma((expert_ranks,)),
                dma((expert_ranks,)),
                dma((2, expert_ranks)),
                dma((local_exp, expert_ranks)),
                dma((BLOCKS, expert_ranks)),
                dma((BLOCKS, expert_ranks)),
                dma((3, 8)),
                dma((3,)),
                dma((2,)),
                dma,
                dma((BLOCKS,)),
                dma,
            ],
            compiler_params=pltpu.CompilerParams(collective_id=0, has_side_effects=True, vmem_limit_bytes=67000000),
        )(
            x_loc,
            jnp.swapaxes(wg_loc, 1, 2),
            jnp.swapaxes(wu_loc, 1, 2),
            wd_loc,
            ids_loc.T,
            gate_loc.T,
        )
        return out[0]

    return jax.shard_map(local_layer, mesh=mesh, in_specs=(row_spec, row_spec, row_spec, P("ep", None, "tp"), P("ep", None, "tp"), P("ep", "tp", None)), out_specs=row_spec, check_vma=False)
```
